128 devices in a mesh: graph: 128 (over z, y, x, core).
Axes of the slice: x: 4, y: 4, z: 4, core: 2. Of those that a mesh axis runs over, the one named last changes fastest.
Arguments:
- node_feats: bfloat16 [131072, 1024], P('graph')
- w_one: float32 [1024, 128], replicated
- w_two: float32 [128, 19], replicated
- send_idx: int32 [256, 512], P('graph')
- edge_src: int32 [2097152], P('graph')
- edge_dst: int32 [2097152], P('graph')
- edge_w: float32 [2097152], P('graph')
- labels: int32 [131072], P('graph')
- label_mask: int32 [131072], P('graph')
Outputs:
- output 1: float32 [], replicated
- output 2: float32 [1024, 128], replicated
- output 3: float32 [128, 19], replicated
All inputs are finite; a program needn't handle non-finite values.
Results may differ from the reference program's by a relative error of at most 0.001.
Values are sent between devices in bfloat16 or wider.
A program may use at most 1 GiB of HBM per device.

```python
import jax
import jax.numpy as jnp
from jax import lax

GRAPH = 128
N_LOC = 1024
HALO = 512
EDGES = 16384
F_IN = 1024
F_HID = 128
CLASSES = 19


def draw_structure(key):
    sub_keys = jax.random.split(key, 9)
    halo_pct = jax.random.randint(sub_keys[0], (GRAPH, 1), 5, 21, jnp.int32)
    pick_draw = jax.random.randint(sub_keys[1], (GRAPH, EDGES), 0, 100, jnp.int32)
    own_src = jax.random.randint(sub_keys[2], (GRAPH, EDGES), 0, N_LOC, jnp.int32)
    halo_src = jax.random.randint(sub_keys[3], (GRAPH, EDGES), N_LOC, N_LOC + 2 * HALO, jnp.int32)
    edge_src = jnp.where(pick_draw < halo_pct, halo_src, own_src)
    edge_dst = jax.random.randint(sub_keys[4], (GRAPH, EDGES), 0, N_LOC, jnp.int32)
    live_count = jax.random.randint(sub_keys[5], (GRAPH, 1), EDGES // 4, EDGES + 1, jnp.int32)
    is_live = jnp.arange(EDGES)[None, :] < live_count
    send_idx = jax.random.randint(sub_keys[6], (GRAPH * 2, HALO), 0, N_LOC, jnp.int32)
    labels = jax.random.randint(sub_keys[7], (GRAPH * N_LOC,), 0, CLASSES, jnp.int32)
    label_mask = jax.random.randint(sub_keys[8], (GRAPH * N_LOC,), 0, 2, jnp.int32)
    return edge_src, edge_dst, is_live, send_idx, labels, label_mask


def normalise(raw_weight, edge_dst):
    weight_sum = jax.vmap(lambda w_g, dst_g: jax.ops.segment_sum(w_g, dst_g, num_segments=N_LOC))(raw_weight, edge_dst)
    node_sum = jnp.take_along_axis(weight_sum, edge_dst, axis=1)
    return raw_weight / jnp.maximum(node_sum, 1e-6)


def setup_inputs(seed: int = 0) -> dict:
    key_list = jax.random.split(jax.random.key(seed), 5)
    edge_src, edge_dst, is_live, send_idx, labels, label_mask = draw_structure(key_list[0])
    deg_gain = EDGES / N_LOC
    node_feats = jax.random.normal(key_list[1], (GRAPH * N_LOC, F_IN), jnp.float32)
    w_one = jax.random.normal(key_list[2], (F_IN, F_HID), jnp.float32) * (deg_gain / F_IN) ** 0.5
    w_two = jax.random.normal(key_list[3], (F_HID, CLASSES), jnp.float32) * (deg_gain / F_HID) ** 0.5
    raw_weight = jax.random.uniform(key_list[4], (GRAPH, EDGES), jnp.float32, 0.5, 1.5) * is_live
    edge_w = normalise(raw_weight, edge_dst)
    return {"node_feats": node_feats.astype(jnp.bfloat16), "w_one": w_one, "w_two": w_two, "send_idx": send_idx, "edge_src": edge_src.reshape(-1), "edge_dst": edge_dst.reshape(-1), "edge_w": edge_w.reshape(-1), "labels": labels, "label_mask": label_mask}


def halo_extend(node_table, send_rows):
    pick_rows = jax.vmap(lambda table_g, idx_g: table_g[idx_g])
    from_prev = pick_rows(jnp.roll(node_table, 1, axis=0), jnp.roll(send_rows[:, 1], 1, axis=0))
    from_next = pick_rows(jnp.roll(node_table, -1, axis=0), jnp.roll(send_rows[:, 0], -1, axis=0))
    return jnp.concatenate([node_table, from_prev, from_next], axis=1)


def aggregate(ext_table, src_dev, dst_dev, w_dev):
    def one_device(args_g):
        ext_g, src_g, dst_g, w_g = args_g
        return jax.ops.segment_sum(w_g[:, None] * ext_g[src_g].astype(jnp.float32), dst_g, num_segments=N_LOC)
    return lax.map(one_device, (ext_table, src_dev, dst_dev, w_dev))


def scatter_back(grad_rows, send_rows, src_dev, dst_dev, w_dev):
    def one_device(args_g):
        grad_g, src_g, dst_g, w_g = args_g
        return jax.ops.segment_sum(w_g[:, None] * grad_g[dst_g], src_g, num_segments=N_LOC + 2 * HALO)
    ext_grad = lax.map(one_device, (grad_rows, src_dev, dst_dev, w_dev))
    back_prev = jnp.roll(ext_grad[:, N_LOC:N_LOC + HALO], -1, axis=0)
    back_next = jnp.roll(ext_grad[:, N_LOC + HALO:], 1, axis=0)
    row_ids = jnp.concatenate([send_rows[:, 1], send_rows[:, 0]], axis=1)
    ret_vals = jnp.concatenate([back_prev, back_next], axis=1)
    returned = jax.vmap(lambda vals_g, ids_g: jax.ops.segment_sum(vals_g, ids_g, num_segments=N_LOC))(ret_vals, row_ids)
    return ext_grad[:, :N_LOC] + returned


def reference(node_feats, w_one, w_two, send_idx, edge_src, edge_dst, edge_w, labels, label_mask):
    send_rows = send_idx.reshape(GRAPH, 2, HALO)
    src_dev = edge_src.reshape(GRAPH, EDGES)
    dst_dev = edge_dst.reshape(GRAPH, EDGES)
    w_dev = edge_w.reshape(GRAPH, EDGES)
    w_one_b = w_one.astype(jnp.bfloat16)
    w_two_b = w_two.astype(jnp.bfloat16)
    tab_one = jnp.dot(node_feats, w_one_b, preferred_element_type=jnp.float32).astype(jnp.bfloat16)
    pre_one = aggregate(halo_extend(tab_one.reshape(GRAPH, N_LOC, F_HID), send_rows), src_dev, dst_dev, w_dev).reshape(GRAPH * N_LOC, F_HID)
    hidden = jnp.maximum(pre_one, 0.0).astype(jnp.bfloat16)
    tab_two = jnp.dot(hidden, w_two_b, preferred_element_type=jnp.float32).astype(jnp.bfloat16)
    logits = aggregate(halo_extend(tab_two.reshape(GRAPH, N_LOC, CLASSES), send_rows), src_dev, dst_dev, w_dev).reshape(GRAPH * N_LOC, CLASSES)
    mask_f = label_mask.astype(jnp.float32)
    label_count = jnp.maximum(jnp.sum(mask_f), 1.0)
    log_norm = jax.nn.logsumexp(logits, axis=1)
    one_hot = (labels[:, None] == jnp.arange(CLASSES)[None, :]).astype(jnp.float32)
    picked = jnp.sum(logits * one_hot, axis=1)
    mean_loss = jnp.sum(mask_f * (log_norm - picked)) / label_count
    d_logits = (jnp.exp(logits - log_norm[:, None]) - one_hot) * (mask_f / label_count)[:, None]
    d_tab_two = scatter_back(d_logits.reshape(GRAPH, N_LOC, CLASSES), send_rows, src_dev, dst_dev, w_dev).reshape(GRAPH * N_LOC, CLASSES).astype(jnp.bfloat16)
    grad_two = jnp.dot(hidden.T, d_tab_two, preferred_element_type=jnp.float32)
    d_hidden = jnp.dot(d_tab_two, w_two_b.T, preferred_element_type=jnp.float32)
    d_pre = jnp.where(pre_one > 0.0, d_hidden, 0.0)
    d_tab_one = scatter_back(d_pre.reshape(GRAPH, N_LOC, F_HID), send_rows, src_dev, dst_dev, w_dev).reshape(GRAPH * N_LOC, F_HID).astype(jnp.bfloat16)
    grad_one = jnp.dot(node_feats.T, d_tab_one, preferred_element_type=jnp.float32)
    return mean_loss, grad_one, grad_two
```

```python
import functools

import jax
import jax.numpy as jnp
from jax import lax
from jax.experimental import pallas as pl
from jax.experimental.pallas import tpu as pltpu
from jax.sharding import PartitionSpec as P

AXIS = "graph"
F32 = jnp.float32
BF16 = jnp.bfloat16
NODES = 1024
HALO = 512
EXT = NODES + 2 * HALO
HID = 128
PADC = 32
BATCH = 128
GROUP = 16
NB = 4
ROW_N = (((1,), (0,)), ((), ()))
ROW_T = (((1,), (1,)), ((), ()))


def split3(x):
    high = x.astype(BF16)
    rest = x - high.astype(F32)
    mid = rest.astype(BF16)
    low = (rest - mid.astype(F32)).astype(BF16)
    return high, mid, low


def dot_n(a, b):
    return lax.dot_general(a, b, ROW_N, preferred_element_type=F32)


def dot_t(a, b):
    return lax.dot_general(a, b, ROW_T, preferred_element_type=F32)


def build_kernel(src_ref, dst_ref, w_ref, bh_ref, bm_ref, bl_ref, m_ref, rs0, rs1, row_v, wh, wm, wl, *rest):
    us0, us1, sem = rest[:NB], rest[NB:2 * NB], rest[2 * NB]
    n_batch = src_ref.shape[0]
    row_v[...] = ((dst_ref[...] >> 7) << 11) + src_ref[...]
    h, m, l = split3(w_ref[...])
    wh[...] = h.astype(F32)
    wm[...] = m.astype(F32)
    wl[...] = l.astype(F32)
    n_half = n_batch // NB

    def rows_copy(i, rs, k):
        return pltpu.make_async_copy(row_v.at[pl.ds(pl.multiple_of(i * NB, NB), NB), :], rs, sem.at[k])

    rows_copy(0, rs0, 0).start()

    def zero(i, c):
        m_ref[pl.ds(pl.multiple_of(i * 256, 256), 256), :] = jnp.zeros((256, 128), F32)
        return c

    lax.fori_loop(0, m_ref.shape[0] // 256, zero, 0)
    ii = lax.broadcasted_iota(jnp.int32, (BATCH, BATCH), 1)
    jj = lax.broadcasted_iota(jnp.int32, (BATCH, BATCH), 0)
    tri = jnp.logical_and(ii <= jj, (ii >> 4) == (jj >> 4))

    def make_u(b, u):
        rb = jnp.broadcast_to(row_v[pl.ds(b, 1), :], (BATCH, BATCH))
        same = jnp.where(jnp.logical_and(rb == rb.T, tri), 1.0, 0.0).astype(BF16)
        hit = jj == (dst_ref[pl.ds(b, 1), :] & 127)
        acc = None
        for piece in (wh, wm, wl):
            v = jnp.where(hit, piece[pl.ds(b, 1), :], 0.0).astype(BF16)
            d = dot_t(same, v)
            acc = d if acc is None else acc + d
        u[...] = acc

    def rmw(k, rs, u):
        for g in range(BATCH // GROUP):
            rows = [rs[k, g * GROUP + j] for j in range(GROUP)]
            vals = [m_ref[pl.ds(rows[j], 1), :] + u[pl.ds(g * GROUP + j, 1), :] for j in range(GROUP)]
            for j in range(GROUP):
                m_ref[pl.ds(rows[j], 1), :] = vals[j]

    for k in range(NB):
        make_u(k, us0[k])

    def body(t, c):
        b = 2 * NB * t
        rows_copy(2 * t, rs0, 0).wait()
        rows_copy(2 * t + 1, rs1, 1).start()
        for k in range(NB):
            make_u(b + NB + k, us1[k])
        for k in range(NB):
            rmw(k, rs0, us0[k])
        rows_copy(2 * t + 1, rs1, 1).wait()
        nxt = jnp.minimum(2 * t + 2, n_half - 1)
        rows_copy(nxt, rs0, 0).start()
        for k in range(NB):
            make_u(nxt * NB + k, us0[k])
        for k in range(NB):
            rmw(k, rs1, us1[k])
        return c

    lax.fori_loop(0, n_half // 2, body, 0)
    rows_copy(n_half - 1, rs0, 0).wait()

    def out(i, c):
        rows = pl.ds(pl.multiple_of(i * 128, 128), 128)
        for j in range(NODES // 128):
            h, m, l = split3(m_ref[pl.ds(pl.multiple_of(j * EXT + i * 128, 128), 128), :])
            cols = pl.ds(j * 128, 128)
            bh_ref[rows, cols] = h
            bm_ref[rows, cols] = m
            bl_ref[rows, cols] = l
        return c

    lax.fori_loop(0, EXT // 128, out, 0)


def build(src, dst, w):
    n = src.shape[0]
    nb = n // BATCH
    piece = jax.ShapeDtypeStruct((EXT, NODES), BF16)
    vmem = pl.BlockSpec(memory_space=pltpu.VMEM)
    return pl.pallas_call(
        build_kernel,
        out_shape=[piece] * 3,
        in_specs=[vmem] * 3,
        out_specs=[vmem] * 3,
        scratch_shapes=[
            pltpu.VMEM((8 * EXT, 128), F32),
            pltpu.SMEM((NB, BATCH), jnp.int32),
            pltpu.SMEM((NB, BATCH), jnp.int32),
            pltpu.VMEM((nb, BATCH), jnp.int32),
        ]
        + [pltpu.VMEM((nb, BATCH), F32)] * 3
        + [pltpu.VMEM((BATCH, 128), F32)] * (2 * NB)
        + [pltpu.SemaphoreType.DMA((2,))],
        name="build",
        compiler_params=pltpu.CompilerParams(vmem_limit_bytes=40 * 1024 * 1024),
    )(src.reshape(nb, BATCH), dst.reshape(nb, BATCH), w.reshape(nb, BATCH))


def step_kernel(
    x_ref, w1_ref, w2t_ref, w2_ref, send_ref, bh_ref, bm_ref, bl_ref, lab_ref, mask_ref,
    loss_ref, out_ref, two_ref,
    s0_ref, s1_ref, sb1, hp1, hn1, sb2, hp2, hn2, gb2, ra2, rb2, gb1, ra1, rb1,
    y_ref, hid_ref, part, rc, a1, rx, a2, ry, a3, rz, cnt, cntr, sml, smlr, own_ref, dy_ref, ssem, rsem,
):
    me = lax.axis_index(AXIS)
    num = 128
    core = lax.rem(me, 2)
    cx = lax.rem(me // 2, 4)
    cy = lax.rem(me // 8, 4)
    cz = me // 32
    nxt = lax.rem(me + 1, num)
    prv = lax.rem(me + num - 1, num)
    twin = me + 1 - 2 * core
    dims = ((cx, 2), (cy, 8), (cz, 32))

    def peer(dim, d):
        c, stride = dims[dim]
        p = lax.rem(c + d, 4)
        return p, me + (p - c) * stride

    barrier = pltpu.get_barrier_semaphore()
    targets = [nxt, prv, twin] + [peer(k, d)[1] for k in range(3) for d in (1, 2, 3)]
    for t in targets:
        pl.semaphore_signal(barrier, inc=1, device_id=(t,), device_id_type=pl.DeviceIdType.MESH)
    pl.semaphore_wait(barrier, len(targets))

    counter = [0]

    def copy(src, dst, dev):
        k = counter[0]
        counter[0] += 1
        c = pltpu.make_async_remote_copy(
            src_ref=src, dst_ref=dst, send_sem=ssem.at[k], recv_sem=rsem.at[k],
            device_id=(dev,), device_id_type=pl.DeviceIdType.MESH,
        )
        c.start()
        return c

    cnt[...] = jnp.broadcast_to(jnp.sum(mask_ref[...].astype(F32), axis=1, keepdims=True), (8, 128))

    def small_start(val, recv, stage):
        if stage == 0:
            return [copy(val, recv.at[0, 0], twin)]
        c, _ = dims[stage - 1]
        recv[stage, c] = val[...]
        return [copy(val, recv.at[stage, c], peer(stage - 1, d)[1]) for d in (1, 2, 3)]

    def small_end(copies, val, recv, stage):
        for c in copies:
            c.wait()
        if stage == 0:
            val[...] = val[...] + recv[0, 0]
        else:
            val[...] = (recv[stage, 0] + recv[stage, 1]) + (recv[stage, 2] + recv[stage, 3])

    cc = small_start(cnt, cntr, 0)

    node = lax.broadcasted_iota(jnp.int32, (NODES, HALO), 0)
    s0_ref[...] = jnp.where(node == send_ref[0:1, :], 1.0, 0.0).astype(BF16)
    s1_ref[...] = jnp.where(node == send_ref[1:2, :], 1.0, 0.0).astype(BF16)

    t1 = dot_n(x_ref[...], w1_ref[...].astype(BF16))
    t1 = t1.T.astype(BF16)
    sb1[1] = dot_n(t1, s1_ref[...]).astype(BF16)
    sb1[0] = dot_n(t1, s0_ref[...]).astype(BF16)
    c_p = copy(sb1.at[1], hp1, nxt)
    c_n = copy(sb1.at[0], hn1, prv)

    def agg(e, lo, hi):
        acc = dot_n(e, bl_ref[lo:hi, :])
        acc = acc + dot_n(e, bm_ref[lo:hi, :])
        return acc + dot_n(e, bh_ref[lo:hi, :])

    y_ref[...] = agg(t1, 0, NODES)
    small_end(cc, cnt, cntr, 0)
    cc = small_start(cnt, cntr, 1)
    c_p.wait()
    c_n.wait()
    y = y_ref[...] + (agg(hp1[...], NODES, NODES + HALO) + agg(hn1[...], NODES + HALO, EXT))
    y_ref[...] = y
    small_end(cc, cnt, cntr, 1)
    cc = small_start(cnt, cntr, 2)
    hid = jnp.maximum(y, 0.0).astype(BF16)
    hid_ref[...] = hid
    t2 = dot_n(w2t_ref[...], hid).astype(BF16)
    sb2[1] = dot_n(t2, s1_ref[...]).astype(BF16)
    sb2[0] = dot_n(t2, s0_ref[...]).astype(BF16)
    c_p = copy(sb2.at[1], hp2, nxt)
    c_n = copy(sb2.at[0], hn2, prv)
    z = agg(t2, 0, NODES)
    small_end(cc, cnt, cntr, 2)
    cc = small_start(cnt, cntr, 3)
    c_p.wait()
    c_n.wait()
    z = z + (agg(hp2[...], NODES, NODES + HALO) + agg(hn2[...], NODES + HALO, EXT))
    small_end(cc, cnt, cntr, 3)
    count = jnp.maximum(cnt[0:1, 0:1], 1.0)

    cls = lax.broadcasted_iota(jnp.int32, (PADC, NODES), 0)
    real = cls < 19
    mask = mask_ref[...].astype(F32)
    zm = jnp.where(real, z, -jnp.inf)
    top = jnp.max(zm, axis=0, keepdims=True)
    norm = jnp.log(jnp.sum(jnp.where(real, jnp.exp(z - top), 0.0), axis=0, keepdims=True)) + top
    hot = (cls == lab_ref[...]).astype(F32)
    picked = jnp.sum(z * hot, axis=0, keepdims=True)
    loss = jnp.sum(mask * (norm - picked), axis=1, keepdims=True)
    dz = (jnp.where(real, jnp.exp(z - norm), 0.0) - hot) * (mask / count)

    def agg_back(d, lo, hi):
        n = d.shape[0]
        dh, dm, dl = split3(d)
        rh = dot_t(jnp.concatenate([dh, dm, dl], axis=0), bh_ref[lo:hi, :])
        rm = dot_t(jnp.concatenate([dh, dm], axis=0), bm_ref[lo:hi, :])
        rl = dot_t(dh, bl_ref[lo:hi, :])
        return rh[0:n] + ((rh[n:2 * n] + rm[0:n]) + (rh[2 * n:3 * n] + (rm[n:2 * n] + rl)))

    def returned(r, s_ref):
        n = r.shape[0]
        t = dot_t(jnp.concatenate(split3(r), axis=0), s_ref[...])
        return t[0:n] + (t[n:2 * n] + t[2 * n:3 * n])

    gb2[0] = agg_back(dz, NODES, NODES + HALO)
    c_p = copy(gb2.at[0], ra2, prv)
    gb2[1] = agg_back(dz, NODES + HALO, EXT)
    c_n = copy(gb2.at[1], rb2, nxt)
    own = agg_back(dz, 0, NODES)
    c_p.wait()
    c_n.wait()
    dt2 = (own + (returned(ra2[...], s1_ref) + returned(rb2[...], s0_ref))).astype(BF16)
    g2 = dot_t(dt2, hid_ref[...])
    sml[...] = g2
    sml[24:32, :] = jnp.broadcast_to(loss, (8, 128))
    cs = small_start(sml, smlr, 0)
    dh = dot_n(w2_ref[...], dt2)
    dy_ref[...] = jnp.where(y_ref[...] > 0.0, dh, 0.0)
    gb1[0] = agg_back(dy_ref[...], NODES, NODES + HALO)
    c_p = copy(gb1.at[0], ra1, prv)
    gb1[1] = agg_back(dy_ref[...], NODES + HALO, EXT)
    c_n = copy(gb1.at[1], rb1, nxt)
    small_end(cs, sml, smlr, 0)
    cs = small_start(sml, smlr, 1)
    own_ref[...] = agg_back(dy_ref[...], 0, NODES)
    small_end(cs, sml, smlr, 1)
    cs = small_start(sml, smlr, 2)
    c_p.wait()
    c_n.wait()
    dt1 = (own_ref[...] + (returned(ra1[...], s1_ref) + returned(rb1[...], s0_ref))).astype(BF16)
    small_end(cs, sml, smlr, 2)
    cs = small_start(sml, smlr, 3)
    part[...] = dot_n(dt1, x_ref[...]).T

    mine = pl.ds(pl.multiple_of(core * 512, 512), 512)
    other = pl.ds(pl.multiple_of((1 - core) * 512, 512), 512)
    copy(part.at[other], rc, twin).wait()
    a1[...] = part[mine, :] + rc[...]

    def scatter_stage(dim, val, recv, size, res):
        c, _ = dims[dim]
        cps = []
        for d in (1, 2, 3):
            p, dev = peer(dim, d)
            cps.append(copy(val.at[pl.ds(pl.multiple_of(p * size, size), size)], recv.at[d - 1], dev))
        for k in cps:
            k.wait()
        res[...] = (val[pl.ds(pl.multiple_of(c * size, size), size), :] + recv[0]) + (recv[1] + recv[2])

    scatter_stage(0, a1, rx, 128, a2)
    small_end(cs, sml, smlr, 3)
    scatter_stage(1, a2, ry, 32, a3)
    spot = core * 512 + cx * 128 + cy * 32 + cz * 8
    scatter_stage(2, a3, rz, 8, out_ref.at[pl.ds(pl.multiple_of(spot, 8), 8)])

    def gather_stage(dim, start, size):
        rows = out_ref.at[pl.ds(pl.multiple_of(start, size), size)]
        cps = [copy(rows, rows, peer(dim, d)[1]) for d in (1, 2, 3)]
        for k in cps:
            k.wait()

    gather_stage(2, spot, 8)
    gather_stage(1, core * 512 + cx * 128 + cy * 32, 32)
    gather_stage(0, core * 512 + cx * 128, 128)
    half = out_ref.at[mine]
    last = copy(half, half, twin)
    loss_ref[...] = sml[24:25, 0:1] / count
    two_ref[...] = sml[...].T[:, 0:19]
    last.wait()


def step(x, w_one, w_two, send_rows, src, dst, w, labels, mask):
    bh, bm, bl = build(src, dst, w)
    w2 = w_two.astype(BF16)
    w2t = jnp.zeros((PADC, HID), BF16).at[:19, :].set(w2.T)
    w2p = jnp.zeros((HID, PADC), BF16).at[:, :19].set(w2)
    vmem = pl.BlockSpec(memory_space=pltpu.VMEM)
    n_sem = 10 + 4 + 4 + 10 + 20
    V = pltpu.VMEM
    loss, one, two = pl.pallas_call(
        step_kernel,
        out_shape=[
            jax.ShapeDtypeStruct((1, 1), F32),
            jax.ShapeDtypeStruct((1024, HID), F32),
            jax.ShapeDtypeStruct((HID, 19), F32),
        ],
        in_specs=[vmem] * 10,
        out_specs=[vmem] * 3,
        scratch_shapes=[
            V((NODES, HALO), BF16), V((NODES, HALO), BF16),
            V((2, HID, HALO), BF16), V((HID, HALO), BF16), V((HID, HALO), BF16),
            V((2, PADC, HALO), BF16), V((PADC, HALO), BF16), V((PADC, HALO), BF16),
            V((2, PADC, HALO), F32), V((PADC, HALO), F32), V((PADC, HALO), F32),
            V((2, HID, HALO), F32), V((HID, HALO), F32), V((HID, HALO), F32),
            V((HID, NODES), F32), V((HID, NODES), BF16),
            V((1024, HID), F32), V((512, HID), F32), V((512, HID), F32),
            V((3, 128, HID), F32), V((128, HID), F32), V((3, 32, HID), F32), V((32, HID), F32), V((3, 8, HID), F32),
            V((8, 128), F32), V((4, 4, 8, 128), F32), V((PADC, 128), F32), V((4, 4, PADC, 128), F32),
            V((HID, NODES), F32), V((HID, NODES), F32),
            pltpu.SemaphoreType.DMA((n_sem,)), pltpu.SemaphoreType.DMA((n_sem,)),
        ],
        name="step",
        compiler_params=pltpu.CompilerParams(
            collective_id=0, has_side_effects=True, vmem_limit_bytes=56 * 1024 * 1024
        ),
    )(x, w_one, w2t, w2p, send_rows, bh, bm, bl, labels.reshape(1, NODES), mask.reshape(1, NODES))
    return loss.reshape(()), one, two


def solution(mesh):
    row = P(AXIS)
    return jax.shard_map(
        step, mesh=mesh, in_specs=(row, P(), P(), row, row, row, row, row, row),
        out_specs=(P(), P(), P()), check_vma=False,
    )
```

```python
import functools

import jax
import jax.numpy as jnp
from jax import lax
from jax.experimental import pallas as pl
from jax.experimental.pallas import tpu as pltpu
from jax.sharding import PartitionSpec as P

AXIS = "graph"
F32 = jnp.float32
BF16 = jnp.bfloat16
NODES = 1024
HALO = 512
EXT = NODES + 2 * HALO
HID = 128
PADC = 32
LAST = 8 * EXT
NSM = 4
ROW_N = (((1,), (0,)), ((), ()))
ROW_T = (((1,), (1,)), ((), ()))


def split3(x):
    high = x.astype(BF16)
    rest = x - high.astype(F32)
    mid = rest.astype(BF16)
    low = (rest - mid.astype(F32)).astype(BF16)
    return high, mid, low


def dot_n(a, b):
    return lax.dot_general(a, b, ROW_N, preferred_element_type=F32)


def dot_t(a, b):
    return lax.dot_general(a, b, ROW_T, preferred_element_type=F32)


def build_kernel(src_hbm, dst_hbm, w_hbm, bh_ref, bm_ref, bl_ref, ma, mb, src_v, dst_v, w_v, row_v, lane_v, lane2_v, w2_v, left_v, ua, ub, *rest):
    rss, sem, rsem = rest[:NSM], rest[NSM], rest[NSM + 1]
    tiles = src_v.shape[0] // 8
    loads = [pltpu.make_async_copy(a, b, sem.at[k]) for k, (a, b) in enumerate(((src_hbm, src_v), (dst_hbm, dst_v), (w_hbm, w_v)))]
    for c in loads: c.start()
    def zero(i, c):
        z = jnp.zeros((256, 128), F32)
        rows = pl.ds(pl.multiple_of(i * 256, 256), 256)
        ma[rows, :] = z; mb[rows, :] = z
        return c
    lax.fori_loop(0, LAST // 256, zero, 0)
    for c in loads: c.wait()
    sub = lax.broadcasted_iota(jnp.int32, (8, 128), 0)
    def prep(t, left):
        tile = pl.ds(pl.multiple_of(t * 8, 8), 8)
        dst = dst_v[tile, :]
        row = ((dst >> 7) << 11) + src_v[tile, :]
        lane = (dst & 127).astype(F32)
        w = w_v[tile, :]
        seen = jnp.zeros((8, 128), F32); lane2 = seen; w2 = seen
        for d in range(1, 8):
            same = jnp.logical_and(row == pltpu.roll(row, d, axis=0), sub >= d)
            seen = seen + jnp.where(same, 1.0, 0.0)
            lane2 = lane2 + jnp.where(same, pltpu.roll(lane, d, axis=0), 0.0)
            w2 = w2 + jnp.where(same, pltpu.roll(w, d, axis=0), 0.0)
        late = seen > 1.5
        row_v[tile, :] = jnp.where(late, LAST, row)
        lane_v[tile, :] = lane
        lane2_v[tile, :] = lane2
        w2_v[tile, :] = w2
        mark = jnp.where(late, 1.0, 0.0)
        left_v[tile, :] = mark
        return left + mark
    left = lax.fori_loop(0, tiles, prep, jnp.zeros((8, 128), F32))
    n_left = jnp.sum(left)

    def rows_copy(t, rs, k):
        return pltpu.make_async_copy(row_v.at[pl.ds(pl.multiple_of(t * 8, 8), 8), :], rs, rsem.at[k])
    lanes = lax.broadcasted_iota(jnp.int32, (128, 128), 1).astype(F32)
    def cols(t):
        tile = pl.ds(pl.multiple_of(t * 8, 8), 8)
        return [r[tile, :].T for r in (lane_v, w_v, lane2_v, w2_v)]
    def make_u(cs, k, u):
        l1, w1, l2, w2 = [jnp.broadcast_to(c[:, k:k + 1], (128, 128)) for c in cs]
        u[k] = jnp.where(lanes == l1, w1, 0.0) + jnp.where(lanes == l2, w2, 0.0)
    def rmw_half(rs, u, hooks):
        pend = None
        for j in range(129):
            if j < 128:
                m = ma if j % 2 == 0 else mb
                rows = [rs[k, j] for k in range(8)]
                vals = [m[pl.ds(rows[k], 1), :] + u[k, pl.ds(j, 1), :] for k in range(8)]
            if pend is not None:
                pm, prow, pval = pend
                for k in range(8):
                    pm[pl.ds(prow[k], 1), :] = pval[k]
            if j < 128:
                pend = (m, rows, vals)
                if j % 16 == 0 and hooks: hooks[j // 16]()
    def half(t, nxt, cur_u, nxt_u, cur_rs):
        cs = cols(nxt)
        hooks = [functools.partial(make_u, cs, k, nxt_u) for k in range(8)]
        rmw_half(cur_rs, cur_u, hooks)
    cs = cols(0)
    for k in range(8): make_u(cs, k, ua)
    NS = len(rss)
    for q in range(NS - 1): rows_copy(q, rss[q], q).start()
    def body(i, c):
        for q in range(NS):
            t = NS * i + q
            rows_copy(t, rss[q], q).wait()
            rows_copy(jnp.minimum(t + NS - 1, tiles - 1), rss[(q + NS - 1) % NS], (q + NS - 1) % NS).start()
            half(t, jnp.minimum(t + 1, tiles - 1), (ua, ub)[q % 2], (ub, ua)[q % 2], rss[q])
        return c
    lax.fori_loop(0, tiles // NS, body, 0)
    for q in range(NS - 1): rows_copy(tiles - 1, rss[q], q).wait()

    pos = lax.broadcasted_iota(jnp.int32, (8 * tiles, 128), 0) * 128 + lax.broadcasted_iota(jnp.int32, (8 * tiles, 128), 1)
    lane_row = lax.broadcasted_iota(jnp.int32, (1, 128), 1)
    def one_left(i, c):
        p = jnp.min(jnp.where(left_v[...] > 0.5, pos, 8 * tiles * 128).astype(F32)).astype(jnp.int32)
        here = pos == p
        left_v[...] = jnp.where(here, 0.0, left_v[...])
        pick = lambda x: jnp.sum(jnp.where(here, x, 0.0))
        dst = pick(dst_v[...].astype(F32)).astype(jnp.int32)
        row = ((dst >> 7) << 11) + pick(src_v[...].astype(F32)).astype(jnp.int32)
        ma[pl.ds(row, 1), :] = ma[pl.ds(row, 1), :] + jnp.where(lane_row == (dst & 127), pick(w_v[...]), 0.0)
        return c
    lax.fori_loop(0, n_left.astype(jnp.int32), one_left, 0)

    def out(i, c):
        rows = pl.ds(pl.multiple_of(i * 128, 128), 128)
        for j in range(NODES // 128):
            part = pl.ds(pl.multiple_of(j * EXT + i * 128, 128), 128)
            h, m, l = split3(ma[part, :] + mb[part, :])
            cols = pl.ds(j * 128, 128)
            bh_ref[rows, cols] = h; bm_ref[rows, cols] = m; bl_ref[rows, cols] = l
        return c
    lax.fori_loop(0, EXT // 128, out, 0)
def build(src,dst,w):
    n=src.shape[0]; nb=n//128
    s2=lambda a:pltpu.with_memory_space_constraint(a.reshape(nb,128), pltpu.HBM)
    o=jax.ShapeDtypeStruct((EXT,NODES),BF16)
    V=pl.BlockSpec(memory_space=pltpu.VMEM); H=pl.BlockSpec(memory_space=pltpu.HBM)
    S=pltpu.VMEM
    return pl.pallas_call(build_kernel, out_shape=[o]*3, in_specs=[H]*3, out_specs=[V]*3,
        scratch_shapes=[S((LAST+8,128),F32)]*2+[S((nb,128),jnp.int32)]*2+[S((nb,128),F32)]+[S((nb,128),jnp.int32)]+[S((nb,128),F32)]*4
          +[S((8,128,128),F32)]*2+[pltpu.SMEM((8,128),jnp.int32)]*NSM+[pltpu.SemaphoreType.DMA((3,)),pltpu.SemaphoreType.DMA((NSM,))],
        name="build", cost_estimate=pl.CostEstimate(flops=10**10, bytes_accessed=80 * 10**6, transcendentals=0), compiler_params=pltpu.CompilerParams(vmem_limit_bytes=36*1024*1024))(s2(src),s2(dst),s2(w))


def step_kernel(
    x_ref, w1_ref, w2_ref, send_ref, bh_ref, bm_ref, bl_ref, lab_ref, mask_ref,
    loss_ref, out_ref, two_ref,
    s0_ref, s1_ref, sb1, hp1, hn1, sb2, hp2, hn2, gb2, ra2, rb2, gb1, ra1, rb1,
    y_ref, hid_ref, part, rc, a1, rx, a2, ry, a3, rz, cnt, cntr, sml, smlr, own_ref, dy_ref, w2p, ssem, rsem,
):
    me = lax.axis_index(AXIS)
    num = 128
    core = lax.rem(me, 2)
    cx = lax.rem(me // 2, 4)
    cy = lax.rem(me // 8, 4)
    cz = me // 32
    nxt = lax.rem(me + 1, num)
    prv = lax.rem(me + num - 1, num)
    twin = me + 1 - 2 * core
    dims = ((cx, 2), (cy, 8), (cz, 32))

    def peer(dim, d):
        c, stride = dims[dim]
        p = lax.rem(c + d, 4)
        return p, me + (p - c) * stride

    barrier = pltpu.get_barrier_semaphore()
    targets = [nxt, prv, twin] + [peer(k, d)[1] for k in range(3) for d in (1, 2, 3)]
    for t in targets:
        pl.semaphore_signal(barrier, inc=1, device_id=(t,), device_id_type=pl.DeviceIdType.MESH)
    pl.semaphore_wait(barrier, len(targets))

    counter = [0]

    def copy(src, dst, dev):
        k = counter[0]
        counter[0] += 1
        c = pltpu.make_async_remote_copy(
            src_ref=src, dst_ref=dst, send_sem=ssem.at[k], recv_sem=rsem.at[k],
            device_id=(dev,), device_id_type=pl.DeviceIdType.MESH,
        )
        c.start()
        return c

    cnt[...] = jnp.broadcast_to(jnp.sum(mask_ref[...].astype(F32), axis=1, keepdims=True), (8, 128))

    def small_start(val, recv, stage):
        if stage == 0:
            return [copy(val, recv.at[0, 0], twin)]
        c, _ = dims[stage - 1]
        recv[stage, c] = val[...]
        return [copy(val, recv.at[stage, c], peer(stage - 1, d)[1]) for d in (1, 2, 3)]

    def small_end(copies, val, recv, stage):
        for c in copies:
            c.wait()
        if stage == 0:
            val[...] = val[...] + recv[0, 0]
        else:
            val[...] = (recv[stage, 0] + recv[stage, 1]) + (recv[stage, 2] + recv[stage, 3])

    cc = small_start(cnt, cntr, 0)

    w2p[...] = jnp.zeros((HID, HID), F32)
    w2p[:, 0:19] = w2_ref[...]
    w2t = w2p[...].T.astype(BF16)[0:PADC, :]

    node = lax.broadcasted_iota(jnp.int32, (NODES, HALO), 0)
    s0_ref[...] = jnp.where(node == send_ref[0:1, :], 1.0, 0.0).astype(BF16)
    s1_ref[...] = jnp.where(node == send_ref[1:2, :], 1.0, 0.0).astype(BF16)

    t1 = dot_n(x_ref[...], w1_ref[...].astype(BF16))
    t1 = t1.T.astype(BF16)
    sb1[1] = dot_n(t1, s1_ref[...]).astype(BF16)
    sb1[0] = dot_n(t1, s0_ref[...]).astype(BF16)
    c_p = copy(sb1.at[1], hp1, nxt)
    c_n = copy(sb1.at[0], hn1, prv)

    def agg(e, lo, hi):
        acc = dot_n(e, bl_ref[lo:hi, :])
        acc = acc + dot_n(e, bm_ref[lo:hi, :])
        return acc + dot_n(e, bh_ref[lo:hi, :])

    y_ref[...] = agg(t1, 0, NODES)
    small_end(cc, cnt, cntr, 0)
    cc = small_start(cnt, cntr, 1)
    c_p.wait()
    c_n.wait()
    y = y_ref[...] + (agg(hp1[...], NODES, NODES + HALO) + agg(hn1[...], NODES + HALO, EXT))
    y_ref[...] = y
    small_end(cc, cnt, cntr, 1)
    cc = small_start(cnt, cntr, 2)
    hid = jnp.maximum(y, 0.0).astype(BF16)
    hid_ref[...] = hid
    t2 = dot_n(w2t, hid).astype(BF16)
    sb2[1] = dot_n(t2, s1_ref[...]).astype(BF16)
    sb2[0] = dot_n(t2, s0_ref[...]).astype(BF16)
    c_p = copy(sb2.at[1], hp2, nxt)
    c_n = copy(sb2.at[0], hn2, prv)
    z = agg(t2, 0, NODES)
    small_end(cc, cnt, cntr, 2)
    cc = small_start(cnt, cntr, 3)
    c_p.wait()
    c_n.wait()
    z = z + (agg(hp2[...], NODES, NODES + HALO) + agg(hn2[...], NODES + HALO, EXT))
    small_end(cc, cnt, cntr, 3)
    count = jnp.maximum(cnt[0:1, 0:1], 1.0)

    cls = lax.broadcasted_iota(jnp.int32, (PADC, NODES), 0)
    real = cls < 19
    mask = mask_ref[...].astype(F32)
    zm = jnp.where(real, z, -jnp.inf)
    top = jnp.max(zm, axis=0, keepdims=True)
    norm = jnp.log(jnp.sum(jnp.where(real, jnp.exp(z - top), 0.0), axis=0, keepdims=True)) + top
    hot = (cls == lab_ref[...]).astype(F32)
    picked = jnp.sum(z * hot, axis=0, keepdims=True)
    loss = jnp.sum(mask * (norm - picked), axis=1, keepdims=True)
    dz = (jnp.where(real, jnp.exp(z - norm), 0.0) - hot) * (mask / count)

    def agg_back(d, lo, hi):
        n = d.shape[0]
        dh, dm, dl = split3(d)
        rh = dot_t(jnp.concatenate([dh, dm, dl], axis=0), bh_ref[lo:hi, :])
        rm = dot_t(jnp.concatenate([dh, dm], axis=0), bm_ref[lo:hi, :])
        rl = dot_t(dh, bl_ref[lo:hi, :])
        return rh[0:n] + ((rh[n:2 * n] + rm[0:n]) + (rh[2 * n:3 * n] + (rm[n:2 * n] + rl)))

    def returned(r, s_ref):
        n = r.shape[0]
        t = dot_t(jnp.concatenate(split3(r), axis=0), s_ref[...])
        return t[0:n] + (t[n:2 * n] + t[2 * n:3 * n])

    gb2[0] = agg_back(dz, NODES, NODES + HALO)
    c_p = copy(gb2.at[0], ra2, prv)
    gb2[1] = agg_back(dz, NODES + HALO, EXT)
    c_n = copy(gb2.at[1], rb2, nxt)
    own = agg_back(dz, 0, NODES)
    c_p.wait()
    c_n.wait()
    dt2 = (own + (returned(ra2[...], s1_ref) + returned(rb2[...], s0_ref))).astype(BF16)
    g2 = dot_t(dt2, hid_ref[...])
    sml[...] = g2
    sml[24:32, :] = jnp.broadcast_to(loss, (8, 128))
    cs = small_start(sml, smlr, 0)
    dh = dot_n(w2p[:, 0:PADC].astype(BF16), dt2)
    dy_ref[...] = jnp.where(y_ref[...] > 0.0, dh, 0.0)
    gb1[0] = agg_back(dy_ref[...], NODES, NODES + HALO)
    c_p = copy(gb1.at[0], ra1, prv)
    gb1[1] = agg_back(dy_ref[...], NODES + HALO, EXT)
    c_n = copy(gb1.at[1], rb1, nxt)
    small_end(cs, sml, smlr, 0)
    cs = small_start(sml, smlr, 1)
    own_ref[...] = agg_back(dy_ref[...], 0, NODES)
    small_end(cs, sml, smlr, 1)
    cs = small_start(sml, smlr, 2)
    c_p.wait()
    c_n.wait()
    dt1 = (own_ref[...] + (returned(ra1[...], s1_ref) + returned(rb1[...], s0_ref))).astype(BF16)
    small_end(cs, sml, smlr, 2)
    cs = small_start(sml, smlr, 3)
    part[...] = dot_n(dt1, x_ref[...]).T

    mine = pl.ds(pl.multiple_of(core * 512, 512), 512)
    other = pl.ds(pl.multiple_of((1 - core) * 512, 512), 512)
    copy(part.at[other], rc, twin).wait()
    a1[...] = part[mine, :] + rc[...]

    def scatter_stage(dim, val, recv, size, res):
        c, _ = dims[dim]
        cps = []
        for d in (1, 2, 3):
            p, dev = peer(dim, d)
            cps.append(copy(val.at[pl.ds(pl.multiple_of(p * size, size), size)], recv.at[d - 1], dev))
        for k in cps:
            k.wait()
        res[...] = (val[pl.ds(pl.multiple_of(c * size, size), size), :] + recv[0]) + (recv[1] + recv[2])

    scatter_stage(0, a1, rx, 128, a2)
    small_end(cs, sml, smlr, 3)
    scatter_stage(1, a2, ry, 32, a3)
    spot = core * 512 + cx * 128 + cy * 32 + cz * 8
    scatter_stage(2, a3, rz, 8, out_ref.at[pl.ds(pl.multiple_of(spot, 8), 8)])

    def gather_stage(dim, start, size):
        rows = out_ref.at[pl.ds(pl.multiple_of(start, size), size)]
        cps = [copy(rows, rows, peer(dim, d)[1]) for d in (1, 2, 3)]
        for k in cps:
            k.wait()

    gather_stage(2, spot, 8)
    gather_stage(1, core * 512 + cx * 128 + cy * 32, 32)
    gather_stage(0, core * 512 + cx * 128, 128)
    half = out_ref.at[mine]
    last = copy(half, half, twin)
    loss_ref[...] = sml[24:25, 0:1] / count
    two_ref[...] = sml[0:19, :]
    last.wait()


def step(x, w_one, w_two, send_rows, src, dst, w, labels, mask):
    bh, bm, bl = build(src, dst, w)
    vmem = pl.BlockSpec(memory_space=pltpu.VMEM)
    n_sem = 10 + 4 + 4 + 10 + 20
    V = pltpu.VMEM
    loss, one, two = pl.pallas_call(
        step_kernel,
        out_shape=[
            jax.ShapeDtypeStruct((1, 1), F32),
            jax.ShapeDtypeStruct((1024, HID), F32),
            jax.ShapeDtypeStruct((19, HID), F32),
        ],
        in_specs=[vmem] * 9,
        out_specs=[vmem] * 3,
        scratch_shapes=[
            V((NODES, HALO), BF16), V((NODES, HALO), BF16),
            V((2, HID, HALO), BF16), V((HID, HALO), BF16), V((HID, HALO), BF16),
            V((2, PADC, HALO), BF16), V((PADC, HALO), BF16), V((PADC, HALO), BF16),
            V((2, PADC, HALO), F32), V((PADC, HALO), F32), V((PADC, HALO), F32),
            V((2, HID, HALO), F32), V((HID, HALO), F32), V((HID, HALO), F32),
            V((HID, NODES), F32), V((HID, NODES), BF16),
            V((1024, HID), F32), V((512, HID), F32), V((512, HID), F32),
            V((3, 128, HID), F32), V((128, HID), F32), V((3, 32, HID), F32), V((32, HID), F32), V((3, 8, HID), F32),
            V((8, 128), F32), V((4, 4, 8, 128), F32), V((PADC, 128), F32), V((4, 4, PADC, 128), F32),
            V((HID, NODES), F32), V((HID, NODES), F32), V((HID, HID), F32),
            pltpu.SemaphoreType.DMA((n_sem,)), pltpu.SemaphoreType.DMA((n_sem,)),
        ],
        name="step",
        compiler_params=pltpu.CompilerParams(
            collective_id=0, has_side_effects=True, vmem_limit_bytes=28 * 1024 * 1024
        ),
    )(x, w_one, w_two, send_rows, bh, bm, bl, labels.reshape(1, NODES), mask.reshape(1, NODES))
    return loss.reshape(()), one, two.T


def solution(mesh):
    row = P(AXIS)
    return jax.shard_map(
        step, mesh=mesh, in_specs=(row, P(), P(), row, row, row, row, row, row),
        out_specs=(P(), P(), P()), check_vma=False,
    )
```

```python
import functools

import jax
import jax.numpy as jnp
from jax import lax
from jax.experimental import pallas as pl
from jax.experimental.pallas import tpu as pltpu
from jax.sharding import PartitionSpec as P

AXIS = "graph"
F32 = jnp.float32
BF16 = jnp.bfloat16
NODES = 1024
HALO = 512
EXT = NODES + 2 * HALO
HID = 128
PADC = 32
LAST = 8 * EXT
NSM = 4
CHIPS = 64
ROW_N = (((1,), (0,)), ((), ()))
ROW_T = (((1,), (1,)), ((), ()))


def split3(x):
    high = x.astype(BF16)
    rest = x - high.astype(F32)
    mid = rest.astype(BF16)
    low = (rest - mid.astype(F32)).astype(BF16)
    return high, mid, low


def dot_n(a, b):
    return lax.dot_general(a, b, ROW_N, preferred_element_type=F32)


def dot_t(a, b):
    return lax.dot_general(a, b, ROW_T, preferred_element_type=F32)


def build_kernel(src_hbm, dst_hbm, w_hbm, ma, mb, src_v, dst_v, w_v, row_v, lane_v, lane2_v, w2_v, left_v, ua, ub, *rest):
    rss, sem, rsem = rest[:NSM], rest[NSM], rest[NSM + 1]
    tiles = src_v.shape[0] // 8
    loads = [pltpu.make_async_copy(a, b, sem.at[k]) for k, (a, b) in enumerate(((src_hbm, src_v), (dst_hbm, dst_v), (w_hbm, w_v)))]
    for c in loads: c.start()
    def zero(i, c):
        z = jnp.zeros((256, 128), F32)
        rows = pl.ds(pl.multiple_of(i * 256, 256), 256)
        ma[rows, :] = z; mb[rows, :] = z
        return c
    lax.fori_loop(0, LAST // 256, zero, 0)
    for c in loads: c.wait()
    sub = lax.broadcasted_iota(jnp.int32, (8, 128), 0)
    def prep(t, left):
        tile = pl.ds(pl.multiple_of(t * 8, 8), 8)
        dst = dst_v[tile, :]
        row = ((dst >> 7) << 11) + src_v[tile, :]
        lane = (dst & 127).astype(F32)
        w = w_v[tile, :]
        seen = jnp.zeros((8, 128), F32); lane2 = seen; w2 = seen
        for d in range(1, 8):
            same = jnp.logical_and(row == pltpu.roll(row, d, axis=0), sub >= d)
            seen = seen + jnp.where(same, 1.0, 0.0)
            lane2 = lane2 + jnp.where(same, pltpu.roll(lane, d, axis=0), 0.0)
            w2 = w2 + jnp.where(same, pltpu.roll(w, d, axis=0), 0.0)
        late = seen > 1.5
        row_v[tile, :] = jnp.where(late, LAST, row)
        lane_v[tile, :] = lane
        lane2_v[tile, :] = lane2
        w2_v[tile, :] = w2
        mark = jnp.where(late, 1.0, 0.0)
        left_v[tile, :] = mark
        return left + mark
    left = lax.fori_loop(0, tiles, prep, jnp.zeros((8, 128), F32))
    n_left = jnp.sum(left)

    def rows_copy(t, rs, k):
        return pltpu.make_async_copy(row_v.at[pl.ds(pl.multiple_of(t * 8, 8), 8), :], rs, rsem.at[k])
    lanes = lax.broadcasted_iota(jnp.int32, (128, 128), 1).astype(F32)
    def cols(t):
        tile = pl.ds(pl.multiple_of(t * 8, 8), 8)
        return [r[tile, :].T for r in (lane_v, w_v, lane2_v, w2_v)]
    def make_u(cs, k, u):
        l1, w1, l2, w2 = [jnp.broadcast_to(c[:, k:k + 1], (128, 128)) for c in cs]
        u[k] = jnp.where(lanes == l1, w1, 0.0) + jnp.where(lanes == l2, w2, 0.0)
    def rmw_half(rs, u, hooks):
        pend = None
        for j in range(129):
            if j < 128:
                m = ma if j % 2 == 0 else mb
                rows = [rs[k, j] for k in range(8)]
                vals = [m[pl.ds(rows[k], 1), :] + u[k, pl.ds(j, 1), :] for k in range(8)]
            if pend is not None:
                pm, prow, pval = pend
                for k in range(8):
                    pm[pl.ds(prow[k], 1), :] = pval[k]
            if j < 128:
                pend = (m, rows, vals)
                if j % 16 == 0 and hooks: hooks[j // 16]()
    def half(t, nxt, cur_u, nxt_u, cur_rs):
        cs = cols(nxt)
        hooks = [functools.partial(make_u, cs, k, nxt_u) for k in range(8)]
        rmw_half(cur_rs, cur_u, hooks)
    cs = cols(0)
    for k in range(8): make_u(cs, k, ua)
    NS = len(rss)
    for q in range(NS - 1): rows_copy(q, rss[q], q).start()
    def body(i, c):
        for q in range(NS):
            t = NS * i + q
            rows_copy(t, rss[q], q).wait()
            rows_copy(jnp.minimum(t + NS - 1, tiles - 1), rss[(q + NS - 1) % NS], (q + NS - 1) % NS).start()
            half(t, jnp.minimum(t + 1, tiles - 1), (ua, ub)[q % 2], (ub, ua)[q % 2], rss[q])
        return c
    lax.fori_loop(0, tiles // NS, body, 0)
    for q in range(NS - 1): rows_copy(tiles - 1, rss[q], q).wait()

    pos = lax.broadcasted_iota(jnp.int32, (8 * tiles, 128), 0) * 128 + lax.broadcasted_iota(jnp.int32, (8 * tiles, 128), 1)
    lane_row = lax.broadcasted_iota(jnp.int32, (1, 128), 1)
    def one_left(i, c):
        p = jnp.min(jnp.where(left_v[...] > 0.5, pos, 8 * tiles * 128).astype(F32)).astype(jnp.int32)
        here = pos == p
        left_v[...] = jnp.where(here, 0.0, left_v[...])
        pick = lambda x: jnp.sum(jnp.where(here, x, 0.0))
        dst = pick(dst_v[...].astype(F32)).astype(jnp.int32)
        row = ((dst >> 7) << 11) + pick(src_v[...].astype(F32)).astype(jnp.int32)
        ma[pl.ds(row, 1), :] = ma[pl.ds(row, 1), :] + jnp.where(lane_row == (dst & 127), pick(w_v[...]), 0.0)
        return c
    lax.fori_loop(0, n_left.astype(jnp.int32), one_left, 0)


def build(src,dst,w):
    n=src.shape[0]; nb=n//128
    s2=lambda a:pltpu.with_memory_space_constraint(a.reshape(nb,128), pltpu.HBM)
    o=jax.ShapeDtypeStruct((LAST+8,128),F32)
    V=pl.BlockSpec(memory_space=pltpu.VMEM); H=pl.BlockSpec(memory_space=pltpu.HBM)
    S=pltpu.VMEM
    return pl.pallas_call(build_kernel, out_shape=[o]*2, in_specs=[H]*3, out_specs=[V]*2,
        scratch_shapes=[S((nb,128),jnp.int32)]*2+[S((nb,128),F32)]+[S((nb,128),jnp.int32)]+[S((nb,128),F32)]*4
          +[S((8,128,128),F32)]*2+[pltpu.SMEM((8,128),jnp.int32)]*NSM+[pltpu.SemaphoreType.DMA((3,)),pltpu.SemaphoreType.DMA((NSM,))],
        name="build", cost_estimate=pl.CostEstimate(flops=10**10, bytes_accessed=80 * 10**6, transcendentals=0), compiler_params=pltpu.CompilerParams(vmem_limit_bytes=36*1024*1024))(s2(src),s2(dst),s2(w))


def step_kernel(
    x_ref, w1_ref, w2_ref, send_ref, ma_ref, mb_ref, lab_ref, mask_ref,
    loss_ref, out_ref, two_ref,
    s0_ref, s1_ref, sb1, hp1, hn1, sb2, hp2, hn2, gb2, ra2, rb2, gb1, ra1, rb1,
    y_ref, hid_ref, part, rc, a1, rx, cnt, cntr, sml, smlr, own_ref, dy_ref, w2p, bh_ref, bm_ref, bl_ref, ssem, rsem, fsem, frsem, gsem, grsem,
):
    me = lax.axis_index(AXIS)
    num = 128
    core = lax.rem(me, 2)
    cx = lax.rem(me // 2, 4)
    cy = lax.rem(me // 8, 4)
    cz = me // 32
    nxt = lax.rem(me + 1, num)
    prv = lax.rem(me + num - 1, num)
    twin = me + 1 - 2 * core
    dims = ((cx, 2), (cy, 8), (cz, 32))

    def peer(dim, d):
        c, stride = dims[dim]
        p = lax.rem(c + d, 4)
        return p, me + (p - c) * stride

    barrier = pltpu.get_barrier_semaphore()
    targets = [nxt, prv, twin] + [peer(k, d)[1] for k in range(3) for d in (1, 2, 3)]
    for t in targets:
        pl.semaphore_signal(barrier, inc=1, device_id=(t,), device_id_type=pl.DeviceIdType.MESH)

    counter = [0]

    def copy(src, dst, dev):
        k = counter[0]
        counter[0] += 1
        c = pltpu.make_async_remote_copy(
            src_ref=src, dst_ref=dst, send_sem=ssem.at[k], recv_sem=rsem.at[k],
            device_id=(dev,), device_id_type=pl.DeviceIdType.MESH,
        )
        c.start()
        return c

    cnt[...] = jnp.broadcast_to(jnp.sum(mask_ref[...].astype(F32), axis=1, keepdims=True), (8, 128))

    def small_start(val, recv, stage):
        if stage == 0:
            return [copy(val, recv.at[0, 0], twin)]
        c, _ = dims[stage - 1]
        recv[stage, c] = val[...]
        return [copy(val, recv.at[stage, c], peer(stage - 1, d)[1]) for d in (1, 2, 3)]

    def small_end(copies, val, recv, stage):
        for c in copies:
            c.wait()
        if stage == 0:
            val[...] = val[...] + recv[0, 0]
        else:
            val[...] = (recv[stage, 0] + recv[stage, 1]) + (recv[stage, 2] + recv[stage, 3])


    w2p[...] = jnp.zeros((HID, HID), F32)
    w2p[0:19, :] = w2_ref[...]
    w2t = w2p[0:PADC, :].astype(BF16)
    w2n = w2p[...].T.astype(BF16)[:, 0:PADC]

    node = lax.broadcasted_iota(jnp.int32, (NODES, HALO), 0)
    s0_ref[...] = jnp.where(node == send_ref[0:1, :], 1.0, 0.0).astype(BF16)
    s1_ref[...] = jnp.where(node == send_ref[1:2, :], 1.0, 0.0).astype(BF16)

    t1 = dot_n(x_ref[...], w1_ref[...].astype(BF16))
    t1 = t1.T.astype(BF16)
    sb1[1] = dot_n(t1, s1_ref[...]).astype(BF16)
    sb1[0] = dot_n(t1, s0_ref[...]).astype(BF16)
    pl.semaphore_wait(barrier, len(targets))
    c_p = copy(sb1.at[1], hp1, nxt)
    c_n = copy(sb1.at[0], hn1, prv)
    cc = small_start(cnt, cntr, 0)

    def agg(e, lo, hi):
        acc = dot_n(e, bl_ref[lo:hi, :])
        acc = acc + dot_n(e, bm_ref[lo:hi, :])
        return acc + dot_n(e, bh_ref[lo:hi, :])

    def split_rows(i, c):
        rows = pl.ds(pl.multiple_of(i * 128, 128), 128)
        for j in range(NODES // 128):
            part_rows = pl.ds(pl.multiple_of(j * EXT + i * 128, 128), 128)
            h, m, l = split3(ma_ref[part_rows, :] + mb_ref[part_rows, :])
            cols = pl.ds(j * 128, 128)
            bh_ref[rows, cols] = h
            bm_ref[rows, cols] = m
            bl_ref[rows, cols] = l
        return c

    lax.fori_loop(0, NODES // 128, split_rows, 0)
    y_ref[...] = agg(t1, 0, NODES)
    lax.fori_loop(NODES // 128, EXT // 128, split_rows, 0)
    small_end(cc, cnt, cntr, 0)
    cc = small_start(cnt, cntr, 1)
    c_p.wait()
    c_n.wait()
    y = y_ref[...] + (agg(hp1[...], NODES, NODES + HALO) + agg(hn1[...], NODES + HALO, EXT))
    y_ref[...] = y
    small_end(cc, cnt, cntr, 1)
    cc = small_start(cnt, cntr, 2)
    hid = jnp.maximum(y, 0.0).astype(BF16)
    hid_ref[...] = hid
    t2 = dot_n(w2t, hid).astype(BF16)
    sb2[1] = dot_n(t2, s1_ref[...]).astype(BF16)
    sb2[0] = dot_n(t2, s0_ref[...]).astype(BF16)
    c_p = copy(sb2.at[1], hp2, nxt)
    c_n = copy(sb2.at[0], hn2, prv)
    z = agg(t2, 0, NODES)
    small_end(cc, cnt, cntr, 2)
    cc = small_start(cnt, cntr, 3)
    c_p.wait()
    c_n.wait()
    z = z + (agg(hp2[...], NODES, NODES + HALO) + agg(hn2[...], NODES + HALO, EXT))
    small_end(cc, cnt, cntr, 3)
    count = jnp.maximum(cnt[0:1, 0:1], 1.0)

    cls = lax.broadcasted_iota(jnp.int32, (PADC, NODES), 0)
    real = cls < 19
    mask = mask_ref[...].astype(F32)
    zm = jnp.where(real, z, -jnp.inf)
    top = jnp.max(zm, axis=0, keepdims=True)
    norm = jnp.log(jnp.sum(jnp.where(real, jnp.exp(z - top), 0.0), axis=0, keepdims=True)) + top
    hot = (cls == lab_ref[...]).astype(F32)
    picked = jnp.sum(z * hot, axis=0, keepdims=True)
    loss = jnp.sum(mask * (norm - picked), axis=1, keepdims=True)
    dz = (jnp.where(real, jnp.exp(z - norm), 0.0) - hot) * (mask / count)

    def agg_back(d, lo, hi):
        n = d.shape[0]
        dh, dm, dl = split3(d)
        rh = dot_t(jnp.concatenate([dh, dm, dl], axis=0), bh_ref[lo:hi, :])
        rm = dot_t(jnp.concatenate([dh, dm], axis=0), bm_ref[lo:hi, :])
        rl = dot_t(dh, bl_ref[lo:hi, :])
        return rh[0:n] + ((rh[n:2 * n] + rm[0:n]) + (rh[2 * n:3 * n] + (rm[n:2 * n] + rl)))

    def returned(r, s_ref):
        n = r.shape[0]
        t = dot_t(jnp.concatenate(split3(r), axis=0), s_ref[...])
        return t[0:n] + (t[n:2 * n] + t[2 * n:3 * n])

    gb2[0] = agg_back(dz, NODES, NODES + HALO)
    c_p = copy(gb2.at[0], ra2, prv)
    gb2[1] = agg_back(dz, NODES + HALO, EXT)
    c_n = copy(gb2.at[1], rb2, nxt)
    own = agg_back(dz, 0, NODES)
    c_p.wait()
    c_n.wait()
    dt2 = (own + (returned(ra2[...], s1_ref) + returned(rb2[...], s0_ref))).astype(BF16)
    g2 = dot_t(dt2, hid_ref[...])
    sml[...] = g2
    sml[24:32, :] = jnp.broadcast_to(loss, (8, 128))
    cs = small_start(sml, smlr, 0)
    dh = dot_n(w2n, dt2)
    dy_ref[...] = jnp.where(y_ref[...] > 0.0, dh, 0.0)
    gb1[0] = agg_back(dy_ref[...], NODES, NODES + HALO)
    c_p = copy(gb1.at[0], ra1, prv)
    gb1[1] = agg_back(dy_ref[...], NODES + HALO, EXT)
    c_n = copy(gb1.at[1], rb1, nxt)
    small_end(cs, sml, smlr, 0)
    cs = small_start(sml, smlr, 1)
    own_ref[...] = agg_back(dy_ref[...], 0, NODES)
    small_end(cs, sml, smlr, 1)
    cs = small_start(sml, smlr, 2)
    c_p.wait()
    c_n.wait()
    dt1 = (own_ref[...] + (returned(ra1[...], s1_ref) + returned(rb1[...], s0_ref))).astype(BF16)
    small_end(cs, sml, smlr, 2)
    cs = small_start(sml, smlr, 3)
    part[...] = dot_n(dt1, x_ref[...]).T

    mine = pl.ds(pl.multiple_of(core * 512, 512), 512)
    other = pl.ds(pl.multiple_of((1 - core) * 512, 512), 512)
    copy(part.at[other], rc, twin).wait()
    a1[...] = part[mine, :] + rc[...]

    chip = me // 2

    def rows_of(q):
        return pl.ds(pl.multiple_of(q * 8, 8), 8)

    def far(i):
        d = lax.rem(i + 41, CHIPS - 1) + 1
        q = lax.rem(chip + d, CHIPS)
        return d - 1, q, q * 2 + core

    def scatter_copy(i):
        k, q, dev = far(i)
        return pltpu.make_async_remote_copy(
            src_ref=a1.at[rows_of(q)], dst_ref=rx.at[k], send_sem=fsem.at[k], recv_sem=frsem.at[k],
            device_id=(dev,), device_id_type=pl.DeviceIdType.MESH,
        )

    def gather_copy(i):
        k, q, dev = far(i)
        rows = out_ref.at[pl.ds(pl.multiple_of(core * 512 + chip * 8, 8), 8)]
        return pltpu.make_async_remote_copy(
            src_ref=rows, dst_ref=rows, send_sem=gsem.at[k], recv_sem=grsem.at[k],
            device_id=(dev,), device_id_type=pl.DeviceIdType.MESH,
        )

    def start_all(make):
        def one(i, c):
            make(i).start()
            return c
        lax.fori_loop(0, CHIPS - 1, one, 0)

    def wait_all(make):
        def one(i, c):
            make(i).wait()
            return c
        lax.fori_loop(0, CHIPS - 1, one, 0)

    start_all(scatter_copy)
    small_end(cs, sml, smlr, 3)
    wait_all(scatter_copy)
    total = a1[rows_of(chip), :]
    for k in range(CHIPS - 1):
        total = total + rx[k]
    out_ref[pl.ds(pl.multiple_of(core * 512 + chip * 8, 8), 8), :] = total
    start_all(gather_copy)
    wait_all(gather_copy)
    half = out_ref.at[mine]
    last = copy(half, half, twin)
    loss_ref[...] = sml[24:25, 0:1] / count
    two_ref[...] = sml[0:19, :]
    last.wait()


def step(x, w_one, w_two, send_rows, src, dst, w, labels, mask):
    ma, mb = build(src, dst, w)
    vmem = pl.BlockSpec(memory_space=pltpu.VMEM)
    n_sem = 30
    V = pltpu.VMEM
    loss, one, two = pl.pallas_call(
        step_kernel,
        out_shape=[
            jax.ShapeDtypeStruct((1, 1), F32),
            jax.ShapeDtypeStruct((1024, HID), F32),
            jax.ShapeDtypeStruct((19, HID), F32),
        ],
        in_specs=[vmem] * 8,
        out_specs=[vmem] * 3,
        scratch_shapes=[
            V((NODES, HALO), BF16), V((NODES, HALO), BF16),
            V((2, HID, HALO), BF16), V((HID, HALO), BF16), V((HID, HALO), BF16),
            V((2, PADC, HALO), BF16), V((PADC, HALO), BF16), V((PADC, HALO), BF16),
            V((2, PADC, HALO), F32), V((PADC, HALO), F32), V((PADC, HALO), F32),
            V((2, HID, HALO), F32), V((HID, HALO), F32), V((HID, HALO), F32),
            V((HID, NODES), F32), V((HID, NODES), BF16),
            V((1024, HID), F32), V((512, HID), F32), V((512, HID), F32),
            V((CHIPS - 1, 8, HID), F32),
            V((8, 128), F32), V((4, 4, 8, 128), F32), V((PADC, 128), F32), V((4, 4, PADC, 128), F32),
            V((HID, NODES), F32), V((HID, NODES), F32), V((HID, HID), F32),
            V((EXT, NODES), BF16), V((EXT, NODES), BF16), V((EXT, NODES), BF16),
            pltpu.SemaphoreType.DMA((n_sem,)), pltpu.SemaphoreType.DMA((n_sem,)),
            *[pltpu.SemaphoreType.DMA((CHIPS - 1,))] * 4,
        ],
        name="step",
        compiler_params=pltpu.CompilerParams(
            collective_id=0, has_side_effects=True, vmem_limit_bytes=31 * 1024 * 1024
        ),
    )(x, w_one, w_two.T, send_rows, ma, mb, labels.reshape(1, NODES), mask.reshape(1, NODES))
    return loss.reshape(()), one, two.T


def solution(mesh):
    row = P(AXIS)
    return jax.shard_map(
        step, mesh=mesh, in_specs=(row, P(), P(), row, row, row, row, row, row),
        out_specs=(P(), P(), P()), check_vma=False,
    )
```

```python
import functools

import jax
import jax.numpy as jnp
from jax import lax
from jax.experimental import pallas as pl
from jax.experimental.pallas import tpu as pltpu
from jax.sharding import PartitionSpec as P

AXIS = "graph"
F32 = jnp.float32
BF16 = jnp.bfloat16
NODES = 1024
HALO = 512
QTR = HALO // 2
EXT = NODES + 2 * HALO
HID = 128
PADC = 32
LAST = 8 * EXT
NSM = 4
CHIPS = 64
ROW_N = (((1,), (0,)), ((), ()))
ROW_T = (((1,), (1,)), ((), ()))


def split3(x):
    high = x.astype(BF16)
    rest = x - high.astype(F32)
    mid = rest.astype(BF16)
    low = (rest - mid.astype(F32)).astype(BF16)
    return high, mid, low


def dot_n(a, b):
    return lax.dot_general(a, b, ROW_N, preferred_element_type=F32)


def dot_t(a, b):
    return lax.dot_general(a, b, ROW_T, preferred_element_type=F32)


def build_kernel(src_hbm, dst_hbm, w_hbm, ma, mb, src_v, dst_v, w_v, row_v, lane_v, lane2_v, w2_v, left_v, ua, ub, *rest):
    rss, sem, rsem = rest[:NSM], rest[NSM], rest[NSM + 1]
    tiles = src_v.shape[0] // 8
    loads = [pltpu.make_async_copy(a, b, sem.at[k]) for k, (a, b) in enumerate(((src_hbm, src_v), (dst_hbm, dst_v), (w_hbm, w_v)))]
    for c in loads: c.start()
    def zero(i, c):
        z = jnp.zeros((256, 128), F32)
        rows = pl.ds(pl.multiple_of(i * 256, 256), 256)
        ma[rows, :] = z; mb[rows, :] = z
        return c
    lax.fori_loop(0, LAST // 256, zero, 0)
    for c in loads: c.wait()
    sub = lax.broadcasted_iota(jnp.int32, (8, 128), 0)
    def prep(t, left):
        tile = pl.ds(pl.multiple_of(t * 8, 8), 8)
        dst = dst_v[tile, :]
        row = ((dst >> 7) << 11) + src_v[tile, :]
        lane = (dst & 127).astype(F32)
        w = w_v[tile, :]
        seen = jnp.zeros((8, 128), F32); lane2 = seen; w2 = seen
        for d in range(1, 8):
            same = jnp.logical_and(row == pltpu.roll(row, d, axis=0), sub >= d)
            seen = seen + jnp.where(same, 1.0, 0.0)
            lane2 = lane2 + jnp.where(same, pltpu.roll(lane, d, axis=0), 0.0)
            w2 = w2 + jnp.where(same, pltpu.roll(w, d, axis=0), 0.0)
        late = seen > 1.5
        row_v[tile, :] = jnp.where(late, LAST, row)
        lane_v[tile, :] = lane
        lane2_v[tile, :] = lane2
        w2_v[tile, :] = w2
        mark = jnp.where(late, 1.0, 0.0)
        left_v[tile, :] = mark
        return left + mark
    left = lax.fori_loop(0, tiles, prep, jnp.zeros((8, 128), F32))
    n_left = jnp.sum(left)

    def rows_copy(t, rs, k):
        return pltpu.make_async_copy(row_v.at[pl.ds(pl.multiple_of(t * 8, 8), 8), :], rs, rsem.at[k])
    lanes = lax.broadcasted_iota(jnp.int32, (128, 128), 1).astype(F32)
    def cols(t):
        tile = pl.ds(pl.multiple_of(t * 8, 8), 8)
        return [r[tile, :].T for r in (lane_v, w_v, lane2_v, w2_v)]
    def make_u(cs, k, u):
        l1, w1, l2, w2 = [jnp.broadcast_to(c[:, k:k + 1], (128, 128)) for c in cs]
        u[k] = jnp.where(lanes == l1, w1, 0.0) + jnp.where(lanes == l2, w2, 0.0)
    def rmw_half(rs, u, hooks):
        pend = None
        for j in range(129):
            if j < 128:
                m = ma if j % 2 == 0 else mb
                rows = [rs[k, j] for k in range(8)]
                vals = [m[pl.ds(rows[k], 1), :] + u[k, pl.ds(j, 1), :] for k in range(8)]
            if pend is not None:
                pm, prow, pval = pend
                for k in range(8):
                    pm[pl.ds(prow[k], 1), :] = pval[k]
            if j < 128:
                pend = (m, rows, vals)
                if j % 16 == 0 and hooks: hooks[j // 16]()
    def half(t, nxt, cur_u, nxt_u, cur_rs):
        cs = cols(nxt)
        hooks = [functools.partial(make_u, cs, k, nxt_u) for k in range(8)]
        rmw_half(cur_rs, cur_u, hooks)
    cs = cols(0)
    for k in range(8): make_u(cs, k, ua)
    NS = len(rss)
    for q in range(NS - 1): rows_copy(q, rss[q], q).start()
    def body(i, c):
        for q in range(NS):
            t = NS * i + q
            rows_copy(t, rss[q], q).wait()
            rows_copy(jnp.minimum(t + NS - 1, tiles - 1), rss[(q + NS - 1) % NS], (q + NS - 1) % NS).start()
            half(t, jnp.minimum(t + 1, tiles - 1), (ua, ub)[q % 2], (ub, ua)[q % 2], rss[q])
        return c
    lax.fori_loop(0, tiles // NS, body, 0)
    for q in range(NS - 1): rows_copy(tiles - 1, rss[q], q).wait()

    pos = lax.broadcasted_iota(jnp.int32, (8 * tiles, 128), 0) * 128 + lax.broadcasted_iota(jnp.int32, (8 * tiles, 128), 1)
    lane_row = lax.broadcasted_iota(jnp.int32, (1, 128), 1)
    def one_left(i, c):
        p = jnp.min(jnp.where(left_v[...] > 0.5, pos, 8 * tiles * 128).astype(F32)).astype(jnp.int32)
        here = pos == p
        left_v[...] = jnp.where(here, 0.0, left_v[...])
        pick = lambda x: jnp.sum(jnp.where(here, x, 0.0))
        dst = pick(dst_v[...].astype(F32)).astype(jnp.int32)
        row = ((dst >> 7) << 11) + pick(src_v[...].astype(F32)).astype(jnp.int32)
        ma[pl.ds(row, 1), :] = ma[pl.ds(row, 1), :] + jnp.where(lane_row == (dst & 127), pick(w_v[...]), 0.0)
        return c
    lax.fori_loop(0, n_left.astype(jnp.int32), one_left, 0)


def build(src,dst,w):
    n=src.shape[0]; nb=n//128
    s2=lambda a:pltpu.with_memory_space_constraint(a.reshape(nb,128), pltpu.HBM)
    o=jax.ShapeDtypeStruct((LAST+8,128),F32)
    V=pl.BlockSpec(memory_space=pltpu.VMEM); H=pl.BlockSpec(memory_space=pltpu.HBM)
    S=pltpu.VMEM
    return pl.pallas_call(build_kernel, out_shape=[o]*2, in_specs=[H]*3, out_specs=[V]*2,
        scratch_shapes=[S((nb,128),jnp.int32)]*2+[S((nb,128),F32)]+[S((nb,128),jnp.int32)]+[S((nb,128),F32)]*4
          +[S((8,128,128),F32)]*2+[pltpu.SMEM((8,128),jnp.int32)]*NSM+[pltpu.SemaphoreType.DMA((3,)),pltpu.SemaphoreType.DMA((NSM,))],
        name="build", cost_estimate=pl.CostEstimate(flops=10**10, bytes_accessed=80 * 10**6, transcendentals=0), compiler_params=pltpu.CompilerParams(vmem_limit_bytes=36*1024*1024))(s2(src),s2(dst),s2(w))


def step_kernel(
    x_ref, w1_ref, w2_ref, send_ref, ma_ref, mb_ref, lab_ref, mask_ref,
    loss_ref, out_ref, two_ref,
    s0_ref, s1_ref, sb1, hp1, hn1, sb2, hp2, hn2, gb2, ra2, rb2, gb1, ra1, rb1,
    y_ref, hid_ref, part, rc, a1, rx, cnt, cntr, sml, smlr, own_ref, dy_ref, w2p, bh_ref, bm_ref, bl_ref, ssem, rsem, fsem, frsem, gsem, grsem,
):
    me = lax.axis_index(AXIS)
    num = 128
    core = lax.rem(me, 2)
    cx = lax.rem(me // 2, 4)
    cy = lax.rem(me // 8, 4)
    cz = me // 32
    nxt = lax.rem(me + 1, num)
    prv = lax.rem(me + num - 1, num)
    twin = me + 1 - 2 * core
    dims = ((cx, 2), (cy, 8), (cz, 32))

    def peer(dim, d):
        c, stride = dims[dim]
        p = lax.rem(c + d, 4)
        return p, me + (p - c) * stride

    barrier = pltpu.get_barrier_semaphore()
    targets = [nxt, prv, twin] + [peer(k, d)[1] for k in range(3) for d in (1, 2, 3)]
    for t in targets:
        pl.semaphore_signal(barrier, inc=1, device_id=(t,), device_id_type=pl.DeviceIdType.MESH)

    counter = [0]

    def copy(src, dst, dev):
        k = counter[0]
        counter[0] += 1
        c = pltpu.make_async_remote_copy(
            src_ref=src, dst_ref=dst, send_sem=ssem.at[k], recv_sem=rsem.at[k],
            device_id=(dev,), device_id_type=pl.DeviceIdType.MESH,
        )
        c.start()
        return c

    cnt[...] = jnp.broadcast_to(jnp.sum(mask_ref[...].astype(F32), axis=1, keepdims=True), (8, 128))

    def small_start(val, recv, stage):
        if stage == 0:
            return [copy(val, recv.at[0, 0], twin)]
        c, _ = dims[stage - 1]
        recv[stage, c] = val[...]
        return [copy(val, recv.at[stage, c], peer(stage - 1, d)[1]) for d in (1, 2, 3)]

    def small_end(copies, val, recv, stage):
        for c in copies:
            c.wait()
        if stage == 0:
            val[...] = val[...] + recv[0, 0]
        else:
            val[...] = (recv[stage, 0] + recv[stage, 1]) + (recv[stage, 2] + recv[stage, 3])


    w2p[...] = jnp.zeros((HID, HID), F32)
    w2p[0:19, :] = w2_ref[...]
    w2t = w2p[0:PADC, :].astype(BF16)
    w2n = w2p[...].T.astype(BF16)[:, 0:PADC]

    node = lax.broadcasted_iota(jnp.int32, (NODES, HALO), 0)
    s0_ref[...] = jnp.where(node == send_ref[0:1, :], 1.0, 0.0).astype(BF16)
    s1_ref[...] = jnp.where(node == send_ref[1:2, :], 1.0, 0.0).astype(BF16)

    t1 = dot_n(x_ref[...], w1_ref[...].astype(BF16))
    t1 = t1.T.astype(BF16)
    sb1[1] = dot_n(t1, s1_ref[...]).astype(BF16)
    sb1[0] = dot_n(t1, s0_ref[...]).astype(BF16)
    pl.semaphore_wait(barrier, len(targets))
    c_p = copy(sb1.at[1], hp1, nxt)
    c_n = copy(sb1.at[0], hn1, prv)
    cc = small_start(cnt, cntr, 0)

    def agg(e, lo, hi):
        acc = dot_n(e, bl_ref[lo:hi, :])
        acc = acc + dot_n(e, bm_ref[lo:hi, :])
        return acc + dot_n(e, bh_ref[lo:hi, :])

    def split_rows(i, c):
        rows = pl.ds(pl.multiple_of(i * 128, 128), 128)
        for j in range(NODES // 128):
            part_rows = pl.ds(pl.multiple_of(j * EXT + i * 128, 128), 128)
            h, m, l = split3(ma_ref[part_rows, :] + mb_ref[part_rows, :])
            cols = pl.ds(j * 128, 128)
            bh_ref[rows, cols] = h
            bm_ref[rows, cols] = m
            bl_ref[rows, cols] = l
        return c

    lax.fori_loop(0, NODES // 128, split_rows, 0)
    y_ref[...] = agg(t1, 0, NODES)
    lax.fori_loop(NODES // 128, EXT // 128, split_rows, 0)
    small_end(cc, cnt, cntr, 0)
    cc = small_start(cnt, cntr, 1)
    c_p.wait()
    c_n.wait()
    y = y_ref[...] + (agg(hp1[...], NODES, NODES + HALO) + agg(hn1[...], NODES + HALO, EXT))
    y_ref[...] = y
    small_end(cc, cnt, cntr, 1)
    cc = small_start(cnt, cntr, 2)
    hid = jnp.maximum(y, 0.0).astype(BF16)
    hid_ref[...] = hid
    t2 = dot_n(w2t, hid).astype(BF16)
    sb2[1] = dot_n(t2, s1_ref[...]).astype(BF16)
    sb2[0] = dot_n(t2, s0_ref[...]).astype(BF16)
    c_p = copy(sb2.at[1], hp2, nxt)
    c_n = copy(sb2.at[0], hn2, prv)
    z = agg(t2, 0, NODES)
    small_end(cc, cnt, cntr, 2)
    cc = small_start(cnt, cntr, 3)
    c_p.wait()
    c_n.wait()
    z = z + (agg(hp2[...], NODES, NODES + HALO) + agg(hn2[...], NODES + HALO, EXT))
    small_end(cc, cnt, cntr, 3)
    count = jnp.maximum(cnt[0:1, 0:1], 1.0)

    cls = lax.broadcasted_iota(jnp.int32, (PADC, NODES), 0)
    real = cls < 19
    mask = mask_ref[...].astype(F32)
    zm = jnp.where(real, z, -jnp.inf)
    top = jnp.max(zm, axis=0, keepdims=True)
    norm = jnp.log(jnp.sum(jnp.where(real, jnp.exp(z - top), 0.0), axis=0, keepdims=True)) + top
    hot = (cls == lab_ref[...]).astype(F32)
    picked = jnp.sum(z * hot, axis=0, keepdims=True)
    loss = jnp.sum(mask * (norm - picked), axis=1, keepdims=True)
    dz = (jnp.where(real, jnp.exp(z - norm), 0.0) - hot) * (mask / count)

    def agg_back(d, lo, hi):
        n = d.shape[0]
        dh, dm, dl = split3(d)
        rh = dot_t(jnp.concatenate([dh, dm, dl], axis=0), bh_ref[lo:hi, :])
        rm = dot_t(jnp.concatenate([dh, dm], axis=0), bm_ref[lo:hi, :])
        rl = dot_t(dh, bl_ref[lo:hi, :])
        return rh[0:n] + ((rh[n:2 * n] + rm[0:n]) + (rh[2 * n:3 * n] + (rm[n:2 * n] + rl)))

    def returned(r, s_ref):
        n = r.shape[0]
        t = dot_t(jnp.concatenate(split3(r), axis=0), s_ref[...])
        return t[0:n] + (t[n:2 * n] + t[2 * n:3 * n])

    gb2[0] = agg_back(dz, NODES, NODES + HALO)
    c_p = copy(gb2.at[0], ra2, prv)
    gb2[1] = agg_back(dz, NODES + HALO, EXT)
    c_n = copy(gb2.at[1], rb2, nxt)
    own = agg_back(dz, 0, NODES)
    c_p.wait()
    c_n.wait()
    dt2 = (own + (returned(ra2[...], s1_ref) + returned(rb2[...], s0_ref))).astype(BF16)
    g2 = dot_t(dt2, hid_ref[...])
    sml[...] = g2
    sml[24:32, :] = jnp.broadcast_to(loss, (8, 128))
    cs = small_start(sml, smlr, 0)
    dh = dot_n(w2n, dt2)
    dy_ref[...] = jnp.where(y_ref[...] > 0.0, dh, 0.0)
    back = []
    for h in range(2):
        gb1[0, h] = agg_back(dy_ref[...], NODES + h * QTR, NODES + (h + 1) * QTR)
        back.append(copy(gb1.at[0, h], ra1.at[h], prv))
        gb1[1, h] = agg_back(dy_ref[...], NODES + HALO + h * QTR, NODES + HALO + (h + 1) * QTR)
        back.append(copy(gb1.at[1, h], rb1.at[h], nxt))
    small_end(cs, sml, smlr, 0)
    cs = small_start(sml, smlr, 1)
    own_ref[...] = agg_back(dy_ref[...], 0, NODES)
    small_end(cs, sml, smlr, 1)
    cs = small_start(sml, smlr, 2)
    for h in range(2):
        cols = pl.ds(h * QTR, QTR)
        back[2 * h].wait()
        back[2 * h + 1].wait()
        own_ref[...] += returned(ra1[h], s1_ref.at[:, cols]) + returned(rb1[h], s0_ref.at[:, cols])
    dt1 = own_ref[...].astype(BF16)

    mine = pl.ds(pl.multiple_of(core * 512, 512), 512)
    other = pl.ds(pl.multiple_of((1 - core) * 512, 512), 512)
    part[...] = dot_n(dt1, x_ref[:, other]).T
    swap = copy(part, rc, twin)
    small_end(cs, sml, smlr, 2)
    cs = small_start(sml, smlr, 3)
    own_half = dot_n(dt1, x_ref[:, mine]).T
    swap.wait()
    a1[...] = own_half + rc[...]

    chip = me // 2

    def rows_of(q):
        return pl.ds(pl.multiple_of(q * 8, 8), 8)

    spot = lax.rem(chip, 16)
    mine8 = pl.ds(pl.multiple_of(core * 512 + chip * 8, 8), 8)
    shifts = [(dz, dr) for dz in (2, 1, 3, 0) for dr in range(16) if dz + dr > 0]

    def far(dz, dr):
        q = lax.rem(cz + dz, 4) * 16 + lax.rem(spot + dr, 16)
        return dz * 16 + dr - 1, q, q * 2 + core

    def far_copy(dz, dr, gather):
        k, q, dev = far(dz, dr)
        src = out_ref.at[mine8] if gather else a1.at[rows_of(q)]
        return pltpu.make_async_remote_copy(
            src_ref=src, dst_ref=src if gather else rx.at[k],
            send_sem=(gsem if gather else fsem).at[k], recv_sem=(grsem if gather else frsem).at[k],
            device_id=(dev,), device_id_type=pl.DeviceIdType.MESH,
        )

    scatters = [far_copy(dz, dr, False) for dz, dr in shifts]
    for c in scatters:
        c.start()
    small_end(cs, sml, smlr, 3)
    for c in scatters:
        c.wait()
    total = [a1[rows_of(chip), :]] + [rx[k] for k in range(CHIPS - 1)]
    while len(total) > 1:
        total = [total[k] + total[k + 1] for k in range(0, len(total), 2)]
    out_ref[mine8, :] = total[0]
    gathers = {(dz, dr): far_copy(dz, dr, True) for dz, dr in shifts}
    for c in gathers.values():
        c.start()
    last = []
    for dz in (0, 1, 3, 2):
        for dr in range(16):
            if dz + dr > 0:
                gathers[dz, dr].wait()
        plane = pl.ds(pl.multiple_of(core * 512 + lax.rem(cz - dz + 4, 4) * 128, 128), 128)
        last.append(copy(out_ref.at[plane], out_ref.at[plane], twin))
    loss_ref[...] = sml[24:25, 0:1] / count
    two_ref[...] = sml[0:19, :]
    for c in last:
        c.wait()


def step(x, w_one, w_two, send_rows, src, dst, w, labels, mask):
    ma, mb = build(src, dst, w)
    vmem = pl.BlockSpec(memory_space=pltpu.VMEM)
    n_sem = 36
    V = pltpu.VMEM
    loss, one, two = pl.pallas_call(
        step_kernel,
        out_shape=[
            jax.ShapeDtypeStruct((1, 1), F32),
            jax.ShapeDtypeStruct((1024, HID), F32),
            jax.ShapeDtypeStruct((19, HID), F32),
        ],
        in_specs=[vmem] * 8,
        out_specs=[vmem] * 3,
        scratch_shapes=[
            V((NODES, HALO), BF16), V((NODES, HALO), BF16),
            V((2, HID, HALO), BF16), V((HID, HALO), BF16), V((HID, HALO), BF16),
            V((2, PADC, HALO), BF16), V((PADC, HALO), BF16), V((PADC, HALO), BF16),
            V((2, PADC, HALO), F32), V((PADC, HALO), F32), V((PADC, HALO), F32),
            V((2, 2, HID, QTR), F32), V((2, HID, QTR), F32), V((2, HID, QTR), F32),
            V((HID, NODES), F32), V((HID, NODES), BF16),
            V((512, HID), F32), V((512, HID), F32), V((512, HID), F32),
            V((CHIPS - 1, 8, HID), F32),
            V((8, 128), F32), V((4, 4, 8, 128), F32), V((PADC, 128), F32), V((4, 4, PADC, 128), F32),
            V((HID, NODES), F32), V((HID, NODES), F32), V((HID, HID), F32),
            V((EXT, NODES), BF16), V((EXT, NODES), BF16), V((EXT, NODES), BF16),
            pltpu.SemaphoreType.DMA((n_sem,)), pltpu.SemaphoreType.DMA((n_sem,)),
            *[pltpu.SemaphoreType.DMA((CHIPS - 1,))] * 4,
        ],
        name="step",
        compiler_params=pltpu.CompilerParams(
            collective_id=0, has_side_effects=True, vmem_limit_bytes=31 * 1024 * 1024
        ),
    )(x, w_one, w_two.T, send_rows, ma, mb, labels.reshape(1, NODES), mask.reshape(1, NODES))
    return loss.reshape(()), one, two.T


def solution(mesh):
    row = P(AXIS)
    return jax.shard_map(
        step, mesh=mesh, in_specs=(row, P(), P(), row, row, row, row, row, row),
        out_specs=(P(), P(), P()), check_vma=False,
    )
```

```python
import functools

import jax
import jax.numpy as jnp
from jax import lax
from jax.experimental import pallas as pl
from jax.experimental.pallas import tpu as pltpu
from jax.sharding import PartitionSpec as P

AXIS = "graph"
F32 = jnp.float32
BF16 = jnp.bfloat16
NODES = 1024
HALO = 512
QTR = HALO // 2
EXT = NODES + 2 * HALO
HID = 128
PADC = 32
LAST = 8 * EXT
NSM = 4
CHIPS = 64
ROW_N = (((1,), (0,)), ((), ()))
ROW_T = (((1,), (1,)), ((), ()))


def split3(x):
    high = x.astype(BF16)
    rest = x - high.astype(F32)
    mid = rest.astype(BF16)
    low = (rest - mid.astype(F32)).astype(BF16)
    return high, mid, low


def dot_n(a, b):
    return lax.dot_general(a, b, ROW_N, preferred_element_type=F32)


def dot_t(a, b):
    return lax.dot_general(a, b, ROW_T, preferred_element_type=F32)


def build_kernel(src_hbm, dst_hbm, w_hbm, ma, mb, src_v, dst_v, w_v, row_v, lane_v, lane2_v, w2_v, left_v, ua, ub, *rest):
    rss, sem, rsem = rest[:NSM], rest[NSM], rest[NSM + 1]
    tiles = src_v.shape[0] // 8
    loads = [pltpu.make_async_copy(a, b, sem.at[k]) for k, (a, b) in enumerate(((src_hbm, src_v), (dst_hbm, dst_v), (w_hbm, w_v)))]
    for c in loads: c.start()
    def zero(i, c):
        z = jnp.zeros((256, 128), F32)
        rows = pl.ds(pl.multiple_of(i * 256, 256), 256)
        ma[rows, :] = z; mb[rows, :] = z
        return c
    lax.fori_loop(0, LAST // 256, zero, 0)
    for c in loads: c.wait()
    sub = lax.broadcasted_iota(jnp.int32, (8, 128), 0)
    def prep(t, left):
        tile = pl.ds(pl.multiple_of(t * 8, 8), 8)
        dst = dst_v[tile, :]
        row = ((dst >> 7) << 11) + src_v[tile, :]
        lane = (dst & 127).astype(F32)
        w = w_v[tile, :]
        seen = jnp.zeros((8, 128), F32); lane2 = seen; w2 = seen
        for d in range(1, 8):
            same = jnp.logical_and(row == pltpu.roll(row, d, axis=0), sub >= d)
            seen = seen + jnp.where(same, 1.0, 0.0)
            lane2 = lane2 + jnp.where(same, pltpu.roll(lane, d, axis=0), 0.0)
            w2 = w2 + jnp.where(same, pltpu.roll(w, d, axis=0), 0.0)
        late = seen > 1.5
        row_v[tile, :] = jnp.where(late, LAST, row)
        lane_v[tile, :] = lane
        lane2_v[tile, :] = lane2
        w2_v[tile, :] = w2
        mark = jnp.where(late, 1.0, 0.0)
        left_v[tile, :] = mark
        return left + mark
    left = lax.fori_loop(0, tiles, prep, jnp.zeros((8, 128), F32))
    n_left = jnp.sum(left)

    def rows_copy(t, rs, k):
        return pltpu.make_async_copy(row_v.at[pl.ds(pl.multiple_of(t * 8, 8), 8), :], rs, rsem.at[k])
    lanes = lax.broadcasted_iota(jnp.int32, (128, 128), 1).astype(F32)
    def cols(t):
        tile = pl.ds(pl.multiple_of(t * 8, 8), 8)
        return [r[tile, :].T for r in (lane_v, w_v, lane2_v, w2_v)]
    def make_u(cs, k, u):
        l1, w1, l2, w2 = [jnp.broadcast_to(c[:, k:k + 1], (128, 128)) for c in cs]
        u[k] = jnp.where(lanes == l1, w1, 0.0) + jnp.where(lanes == l2, w2, 0.0)
    def rmw_half(rs, u, hooks):
        pend = None
        for j in range(129):
            if j < 128:
                m = ma if j % 2 == 0 else mb
                rows = [rs[k, j] for k in range(8)]
                vals = [m[pl.ds(rows[k], 1), :] + u[k, pl.ds(j, 1), :] for k in range(8)]
            if pend is not None:
                pm, prow, pval = pend
                for k in range(8):
                    pm[pl.ds(prow[k], 1), :] = pval[k]
            if j < 128:
                pend = (m, rows, vals)
                if j % 16 == 0 and hooks: hooks[j // 16]()
    def half(t, nxt, cur_u, nxt_u, cur_rs):
        cs = cols(nxt)
        hooks = [functools.partial(make_u, cs, k, nxt_u) for k in range(8)]
        rmw_half(cur_rs, cur_u, hooks)
    cs = cols(0)
    for k in range(8): make_u(cs, k, ua)
    NS = len(rss)
    for q in range(NS - 1): rows_copy(q, rss[q], q).start()
    def body(i, c):
        for q in range(NS):
            t = NS * i + q
            rows_copy(t, rss[q], q).wait()
            rows_copy(jnp.minimum(t + NS - 1, tiles - 1), rss[(q + NS - 1) % NS], (q + NS - 1) % NS).start()
            half(t, jnp.minimum(t + 1, tiles - 1), (ua, ub)[q % 2], (ub, ua)[q % 2], rss[q])
        return c
    lax.fori_loop(0, tiles // NS, body, 0)
    for q in range(NS - 1): rows_copy(tiles - 1, rss[q], q).wait()

    pos = lax.broadcasted_iota(jnp.int32, (8 * tiles, 128), 0) * 128 + lax.broadcasted_iota(jnp.int32, (8 * tiles, 128), 1)
    lane_row = lax.broadcasted_iota(jnp.int32, (1, 128), 1)
    def one_left(i, c):
        p = jnp.min(jnp.where(left_v[...] > 0.5, pos, 8 * tiles * 128).astype(F32)).astype(jnp.int32)
        here = pos == p
        left_v[...] = jnp.where(here, 0.0, left_v[...])
        pick = lambda x: jnp.sum(jnp.where(here, x, 0.0))
        dst = pick(dst_v[...].astype(F32)).astype(jnp.int32)
        row = ((dst >> 7) << 11) + pick(src_v[...].astype(F32)).astype(jnp.int32)
        ma[pl.ds(row, 1), :] = ma[pl.ds(row, 1), :] + jnp.where(lane_row == (dst & 127), pick(w_v[...]), 0.0)
        return c
    lax.fori_loop(0, n_left.astype(jnp.int32), one_left, 0)


def build(src,dst,w):
    n=src.shape[0]; nb=n//128
    s2=lambda a:pltpu.with_memory_space_constraint(a.reshape(nb,128), pltpu.HBM)
    o=jax.ShapeDtypeStruct((LAST+8,128),F32)
    V=pl.BlockSpec(memory_space=pltpu.VMEM); H=pl.BlockSpec(memory_space=pltpu.HBM)
    S=pltpu.VMEM
    return pl.pallas_call(build_kernel, out_shape=[o]*2, in_specs=[H]*3, out_specs=[V]*2,
        scratch_shapes=[S((nb,128),jnp.int32)]*2+[S((nb,128),F32)]+[S((nb,128),jnp.int32)]+[S((nb,128),F32)]*4
          +[S((8,128,128),F32)]*2+[pltpu.SMEM((8,128),jnp.int32)]*NSM+[pltpu.SemaphoreType.DMA((3,)),pltpu.SemaphoreType.DMA((NSM,))],
        name="build", cost_estimate=pl.CostEstimate(flops=10**10, bytes_accessed=80 * 10**6, transcendentals=0), compiler_params=pltpu.CompilerParams(vmem_limit_bytes=36*1024*1024))(s2(src),s2(dst),s2(w))


def step_kernel(
    x_ref, w1_ref, w2_ref, send_ref, ma_ref, mb_ref, lab_ref, mask_ref,
    out_ref, small_ref,
    s0_ref, s1_ref, sb1, hp1, hn1, sb2, hp2, hn2, gb2, ra2, rb2, gb1, ra1, rb1,
    y_ref, hid_ref, part, rc, a1, rx, cnt, cntr, sml, smlr, own_ref, dy_ref, w2p, bh_ref, bm_ref, bl_ref, r0_ref, r1_ref, ssem, rsem, fsem, frsem, gsem, grsem,
):
    me = lax.axis_index(AXIS)
    num = 128
    core = lax.rem(me, 2)
    cx = lax.rem(me // 2, 4)
    cy = lax.rem(me // 8, 4)
    cz = me // 32
    nxt = lax.rem(me + 1, num)
    prv = lax.rem(me + num - 1, num)
    twin = me + 1 - 2 * core
    dims = ((cx, 2), (cy, 8), (cz, 32))

    def peer(dim, d):
        c, stride = dims[dim]
        p = lax.rem(c + d, 4)
        return p, me + (p - c) * stride

    barrier = pltpu.get_barrier_semaphore()
    targets = [nxt, prv, twin] + [peer(k, d)[1] for k in range(3) for d in (1, 2, 3)]
    for t in targets:
        pl.semaphore_signal(barrier, inc=1, device_id=(t,), device_id_type=pl.DeviceIdType.MESH)

    counter = [0]

    def copy(src, dst, dev):
        k = counter[0]
        counter[0] += 1
        c = pltpu.make_async_remote_copy(
            src_ref=src, dst_ref=dst, send_sem=ssem.at[k], recv_sem=rsem.at[k],
            device_id=(dev,), device_id_type=pl.DeviceIdType.MESH,
        )
        c.start()
        return c

    cnt[...] = jnp.broadcast_to(jnp.sum(mask_ref[...].astype(F32), axis=1, keepdims=True), (8, 128))

    def small_start(val, recv, stage):
        if stage == 0:
            return [copy(val, recv.at[0, 0], twin)]
        c, _ = dims[stage - 1]
        recv[stage, c] = val[...]
        return [copy(val, recv.at[stage, c], peer(stage - 1, d)[1]) for d in (1, 2, 3)]

    def small_end(copies, val, recv, stage):
        for c in copies:
            c.wait()
        if stage == 0:
            val[...] = val[...] + recv[0, 0]
        else:
            val[...] = (recv[stage, 0] + recv[stage, 1]) + (recv[stage, 2] + recv[stage, 3])


    w2p[...] = jnp.zeros((HID, HID), F32)
    w2p[0:19, :] = w2_ref[...]
    w2t = w2p[0:PADC, :].astype(BF16)
    w2n = w2p[...].T.astype(BF16)[:, 0:PADC]

    node = lax.broadcasted_iota(jnp.int32, (NODES, HALO), 0)
    s0_ref[...] = jnp.where(node == send_ref[0:1, :], 1.0, 0.0).astype(BF16)
    s1_ref[...] = jnp.where(node == send_ref[1:2, :], 1.0, 0.0).astype(BF16)

    t1 = dot_n(x_ref[...], w1_ref[...].astype(BF16))
    t1 = t1.T.astype(BF16)
    sb1[1] = dot_n(t1, s1_ref[...]).astype(BF16)
    sb1[0] = dot_n(t1, s0_ref[...]).astype(BF16)
    pl.semaphore_wait(barrier, len(targets))
    c_p = copy(sb1.at[1], hp1, nxt)
    c_n = copy(sb1.at[0], hn1, prv)
    cc = small_start(cnt, cntr, 0)

    def agg(e, lo, hi):
        acc = dot_n(e, bl_ref[lo:hi, :])
        acc = acc + dot_n(e, bm_ref[lo:hi, :])
        return acc + dot_n(e, bh_ref[lo:hi, :])

    def split_rows(i, c):
        rows = pl.ds(pl.multiple_of(i * 128, 128), 128)
        for j in range(NODES // 128):
            part_rows = pl.ds(pl.multiple_of(j * EXT + i * 128, 128), 128)
            h, m, l = split3(ma_ref[part_rows, :] + mb_ref[part_rows, :])
            cols = pl.ds(j * 128, 128)
            bh_ref[rows, cols] = h
            bm_ref[rows, cols] = m
            bl_ref[rows, cols] = l
        return c

    lax.fori_loop(0, NODES // 128, split_rows, 0)
    y_ref[...] = agg(t1, 0, NODES)
    lax.fori_loop(NODES // 128, EXT // 128, split_rows, 0)
    column = lax.broadcasted_iota(jnp.int32, (HALO, NODES), 1).astype(F32)
    for k, r_ref in ((0, r0_ref), (1, r1_ref)):
        ids = jnp.broadcast_to(send_ref[k:k + 1, :].astype(F32), (8, HALO)).T[:, 0:1]
        r_ref[...] = jnp.where(column == ids, 1.0, 0.0).astype(BF16)
    small_end(cc, cnt, cntr, 0)
    cc = small_start(cnt, cntr, 1)
    c_p.wait()
    c_n.wait()
    y = y_ref[...] + (agg(hp1[...], NODES, NODES + HALO) + agg(hn1[...], NODES + HALO, EXT))
    y_ref[...] = y
    small_end(cc, cnt, cntr, 1)
    cc = small_start(cnt, cntr, 2)
    hid = jnp.maximum(y, 0.0).astype(BF16)
    hid_ref[...] = hid
    t2 = dot_n(w2t, hid).astype(BF16)
    sb2[1] = dot_n(t2, s1_ref[...]).astype(BF16)
    sb2[0] = dot_n(t2, s0_ref[...]).astype(BF16)
    c_p = copy(sb2.at[1], hp2, nxt)
    c_n = copy(sb2.at[0], hn2, prv)
    z = agg(t2, 0, NODES)
    small_end(cc, cnt, cntr, 2)
    cc = small_start(cnt, cntr, 3)
    c_p.wait()
    c_n.wait()
    z = z + (agg(hp2[...], NODES, NODES + HALO) + agg(hn2[...], NODES + HALO, EXT))
    small_end(cc, cnt, cntr, 3)
    count = jnp.maximum(cnt[0:1, 0:1], 1.0)

    cls = lax.broadcasted_iota(jnp.int32, (PADC, NODES), 0)
    real = cls < 19
    mask = mask_ref[...].astype(F32)
    zm = jnp.where(real, z, -jnp.inf)
    top = jnp.max(zm, axis=0, keepdims=True)
    norm = jnp.log(jnp.sum(jnp.where(real, jnp.exp(z - top), 0.0), axis=0, keepdims=True)) + top
    hot = (cls == lab_ref[...]).astype(F32)
    picked = jnp.sum(z * hot, axis=0, keepdims=True)
    loss = jnp.sum(mask * (norm - picked), axis=1, keepdims=True)
    dz = (jnp.where(real, jnp.exp(z - norm), 0.0) - hot) * (mask / count)

    def agg_back(d, lo, hi):
        n = d.shape[0]
        dh, dm, dl = split3(d)
        rh = dot_t(jnp.concatenate([dh, dm, dl], axis=0), bh_ref[lo:hi, :])
        rm = dot_t(jnp.concatenate([dh, dm], axis=0), bm_ref[lo:hi, :])
        rl = dot_t(dh, bl_ref[lo:hi, :])
        return rh[0:n] + ((rh[n:2 * n] + rm[0:n]) + (rh[2 * n:3 * n] + (rm[n:2 * n] + rl)))

    def returned(r, s_rows):
        n = r.shape[0]
        t = dot_n(jnp.concatenate(split3(r), axis=0), s_rows)
        return t[0:n] + (t[n:2 * n] + t[2 * n:3 * n])

    gb2[0] = agg_back(dz, NODES, NODES + HALO)
    c_p = copy(gb2.at[0], ra2, prv)
    gb2[1] = agg_back(dz, NODES + HALO, EXT)
    c_n = copy(gb2.at[1], rb2, nxt)
    own = agg_back(dz, 0, NODES)
    c_p.wait()
    c_n.wait()
    dt2 = (own + (returned(ra2[...], r1_ref[...]) + returned(rb2[...], r0_ref[...]))).astype(BF16)
    g2 = dot_t(dt2, hid_ref[...])
    sml[...] = g2
    sml[24:32, :] = jnp.broadcast_to(loss, (8, 128))
    cs = small_start(sml, smlr, 0)
    dh = dot_n(w2n, dt2)
    dy_ref[...] = jnp.where(y_ref[...] > 0.0, dh, 0.0)
    back = []
    for h in range(2):
        gb1[0, h] = agg_back(dy_ref[...], NODES + h * QTR, NODES + (h + 1) * QTR)
        back.append(copy(gb1.at[0, h], ra1.at[h], prv))
        gb1[1, h] = agg_back(dy_ref[...], NODES + HALO + h * QTR, NODES + HALO + (h + 1) * QTR)
        back.append(copy(gb1.at[1, h], rb1.at[h], nxt))
    small_end(cs, sml, smlr, 0)
    cs = small_start(sml, smlr, 1)
    own_ref[...] = agg_back(dy_ref[...], 0, NODES)
    small_end(cs, sml, smlr, 1)
    cs = small_start(sml, smlr, 2)
    for h in range(2):
        slots = pl.ds(h * QTR, QTR)
        back[2 * h].wait()
        back[2 * h + 1].wait()
        own_ref[...] += returned(ra1[h], r1_ref[slots, :]) + returned(rb1[h], r0_ref[slots, :])
    dt1 = own_ref[...].astype(BF16)

    mine = pl.ds(pl.multiple_of(core * 512, 512), 512)
    other = pl.ds(pl.multiple_of((1 - core) * 512, 512), 512)
    part[...] = dot_n(dt1, x_ref[:, other]).T
    swap = copy(part, rc, twin)
    small_end(cs, sml, smlr, 2)
    cs = small_start(sml, smlr, 3)
    own_half = dot_n(dt1, x_ref[:, mine]).T
    swap.wait()
    a1[...] = own_half + rc[...]

    chip = me // 2

    def rows_of(q):
        return pl.ds(pl.multiple_of(q * 8, 8), 8)

    spot = lax.rem(chip, 16)
    mine8 = pl.ds(pl.multiple_of(core * 512 + chip * 8, 8), 8)
    shifts = [(dz, dr) for dz in (2, 1, 3, 0) for dr in range(16) if dz + dr > 0]

    def far(dz, dr):
        q = lax.rem(cz + dz, 4) * 16 + lax.rem(spot + dr, 16)
        return dz * 16 + dr - 1, q, q * 2 + core

    def far_copy(dz, dr, gather):
        k, q, dev = far(dz, dr)
        src = out_ref.at[mine8] if gather else a1.at[rows_of(q)]
        return pltpu.make_async_remote_copy(
            src_ref=src, dst_ref=src if gather else rx.at[k],
            send_sem=(gsem if gather else fsem).at[k], recv_sem=(grsem if gather else frsem).at[k],
            device_id=(dev,), device_id_type=pl.DeviceIdType.MESH,
        )

    scatters = [far_copy(dz, dr, False) for dz, dr in shifts]
    for c in scatters:
        c.start()
    small_end(cs, sml, smlr, 3)
    for c in scatters:
        c.wait()
    total = [a1[rows_of(chip), :]] + [rx[k] for k in range(CHIPS - 1)]
    while len(total) > 1:
        total = [total[k] + total[k + 1] for k in range(0, len(total), 2)]
    out_ref[mine8, :] = total[0]
    gathers = {(dz, dr): far_copy(dz, dr, True) for dz, dr in shifts}
    for c in gathers.values():
        c.start()
    last = []
    for dz in (0, 1, 3, 2):
        for dr in range(16):
            if dz + dr > 0:
                gathers[dz, dr].wait()
        plane = pl.ds(pl.multiple_of(core * 512 + lax.rem(cz - dz + 4, 4) * 128, 128), 128)
        last.append(copy(out_ref.at[plane], out_ref.at[plane], twin))
    small_ref[...] = sml[...]
    small_ref[24:32, :] = sml[24:32, :] / count
    for c in last:
        c.wait()


def finish_kernel(one_in, small_in, loss_ref, one_ref, two_ref, two_v, sem):
    one = pltpu.make_async_copy(one_in, one_ref, sem.at[0])
    one.start()
    two_v[...] = small_in[0:19, :]
    two = pltpu.make_async_copy(two_v, two_ref, sem.at[1])
    two.start()
    loss_ref[0, 0] = jnp.max(small_in[24:25, :])
    one.wait()
    two.wait()


def finish(one, small):
    vmem = pl.BlockSpec(memory_space=pltpu.VMEM)
    hbm = pl.BlockSpec(memory_space=pltpu.HBM)
    return pl.pallas_call(
        finish_kernel,
        out_shape=[
            jax.ShapeDtypeStruct((1, 1), F32), jax.ShapeDtypeStruct(one.shape, F32), jax.ShapeDtypeStruct((19, HID), F32),
        ],
        in_specs=[vmem] * 2,
        out_specs=[pl.BlockSpec(memory_space=pltpu.SMEM), hbm, hbm],
        scratch_shapes=[pltpu.VMEM((19, HID), F32), pltpu.SemaphoreType.DMA((2,))],
        name="finish",
        compiler_params=pltpu.CompilerParams(vmem_limit_bytes=4 * 1024 * 1024),
    )(one, small)


def step(x, w_one, w_two, send_rows, src, dst, w, labels, mask):
    ma, mb = build(src, dst, w)
    vmem = pl.BlockSpec(memory_space=pltpu.VMEM)
    n_sem = 36
    V = pltpu.VMEM
    one, small = pl.pallas_call(
        step_kernel,
        out_shape=[
            jax.ShapeDtypeStruct((1024, HID), F32),
            jax.ShapeDtypeStruct((PADC, HID), F32),
        ],
        in_specs=[vmem] * 8,
        out_specs=[vmem] * 2,
        scratch_shapes=[
            V((NODES, HALO), BF16), V((NODES, HALO), BF16),
            V((2, HID, HALO), BF16), V((HID, HALO), BF16), V((HID, HALO), BF16),
            V((2, PADC, HALO), BF16), V((PADC, HALO), BF16), V((PADC, HALO), BF16),
            V((2, PADC, HALO), F32), V((PADC, HALO), F32), V((PADC, HALO), F32),
            V((2, 2, HID, QTR), F32), V((2, HID, QTR), F32), V((2, HID, QTR), F32),
            V((HID, NODES), F32), V((HID, NODES), BF16),
            V((512, HID), F32), V((512, HID), F32), V((512, HID), F32),
            V((CHIPS - 1, 8, HID), F32),
            V((8, 128), F32), V((4, 4, 8, 128), F32), V((PADC, 128), F32), V((4, 4, PADC, 128), F32),
            V((HID, NODES), F32), V((HID, NODES), F32), V((HID, HID), F32),
            V((EXT, NODES), BF16), V((EXT, NODES), BF16), V((EXT, NODES), BF16),
            V((HALO, NODES), BF16), V((HALO, NODES), BF16),
            pltpu.SemaphoreType.DMA((n_sem,)), pltpu.SemaphoreType.DMA((n_sem,)),
            *[pltpu.SemaphoreType.DMA((CHIPS - 1,))] * 4,
        ],
        name="step",
        compiler_params=pltpu.CompilerParams(
            collective_id=0, has_side_effects=True, vmem_limit_bytes=31 * 1024 * 1024
        ),
    )(x, w_one, w_two.T, send_rows, ma, mb, labels.reshape(1, NODES), mask.reshape(1, NODES))
    loss, one, two = finish(one, small)
    return loss.reshape(()), one, two.T


def solution(mesh):
    row = P(AXIS)
    return jax.shard_map(
        step, mesh=mesh, in_specs=(row, P(), P(), row, row, row, row, row, row),
        out_specs=(P(), P(), P()), check_vma=False,
    )
```

```python
import functools

import jax
import jax.numpy as jnp
from jax import lax
from jax.experimental import pallas as pl
from jax.experimental.pallas import tpu as pltpu
from jax.sharding import PartitionSpec as P

AXIS = "graph"
F32 = jnp.float32
BF16 = jnp.bfloat16
NODES = 1024
HALO = 512
QTR = HALO // 2
EXT = NODES + 2 * HALO
HID = 128
PADC = 32
LAST = 8 * EXT
NSM = 4
CHIPS = 64
ROW_N = (((1,), (0,)), ((), ()))
ROW_T = (((1,), (1,)), ((), ()))


def split3(x):
    high = x.astype(BF16)
    rest = x - high.astype(F32)
    mid = rest.astype(BF16)
    low = (rest - mid.astype(F32)).astype(BF16)
    return high, mid, low


def dot_n(a, b):
    return lax.dot_general(a, b, ROW_N, preferred_element_type=F32)


def dot_t(a, b):
    return lax.dot_general(a, b, ROW_T, preferred_element_type=F32)


def build_kernel(src_hbm, dst_hbm, w_hbm, ma, mb, src_v, dst_v, w_v, row_v, lane_v, lane2_v, w2_v, left_v, ua, ub, *rest):
    rss, sem, rsem = rest[:NSM], rest[NSM], rest[NSM + 1]
    tiles = src_v.shape[0] // 8
    loads = [pltpu.make_async_copy(a, b, sem.at[k]) for k, (a, b) in enumerate(((src_hbm, src_v), (dst_hbm, dst_v), (w_hbm, w_v)))]
    for c in loads: c.start()
    def zero(i, c):
        z = jnp.zeros((256, 128), F32)
        rows = pl.ds(pl.multiple_of(i * 256, 256), 256)
        ma[rows, :] = z; mb[rows, :] = z
        return c
    lax.fori_loop(0, LAST // 256, zero, 0)
    for c in loads: c.wait()
    sub = lax.broadcasted_iota(jnp.int32, (8, 128), 0)
    def prep(t, left):
        tile = pl.ds(pl.multiple_of(t * 8, 8), 8)
        dst = dst_v[tile, :]
        row = ((dst >> 7) << 11) + src_v[tile, :]
        lane = (dst & 127).astype(F32)
        w = w_v[tile, :]
        seen = jnp.zeros((8, 128), F32); lane2 = seen; w2 = seen
        for d in range(1, 8):
            same = jnp.logical_and(row == pltpu.roll(row, d, axis=0), sub >= d)
            seen = seen + jnp.where(same, 1.0, 0.0)
            lane2 = lane2 + jnp.where(same, pltpu.roll(lane, d, axis=0), 0.0)
            w2 = w2 + jnp.where(same, pltpu.roll(w, d, axis=0), 0.0)
        late = seen > 1.5
        row_v[tile, :] = jnp.where(late, LAST, row)
        lane_v[tile, :] = lane
        lane2_v[tile, :] = lane2
        w2_v[tile, :] = w2
        mark = jnp.where(late, 1.0, 0.0)
        left_v[tile, :] = mark
        return left + mark
    left = lax.fori_loop(0, tiles, prep, jnp.zeros((8, 128), F32))
    n_left = jnp.sum(left)

    def rows_copy(t, rs, k):
        return pltpu.make_async_copy(row_v.at[pl.ds(pl.multiple_of(t * 8, 8), 8), :], rs, rsem.at[k])
    lanes = lax.broadcasted_iota(jnp.int32, (128, 128), 1).astype(F32)
    def cols(t):
        tile = pl.ds(pl.multiple_of(t * 8, 8), 8)
        return [r[tile, :].T for r in (lane_v, w_v, lane2_v, w2_v)]
    def make_u(cs, k, u):
        l1, w1, l2, w2 = [jnp.broadcast_to(c[:, k:k + 1], (128, 128)) for c in cs]
        u[k] = jnp.where(lanes == l1, w1, 0.0) + jnp.where(lanes == l2, w2, 0.0)
    def rmw_half(rs, u, hooks):
        pend = None
        for j in range(129):
            if j < 128:
                m = ma if j % 2 == 0 else mb
                rows = [rs[k, j] for k in range(8)]
                vals = [m[pl.ds(rows[k], 1), :] + u[k, pl.ds(j, 1), :] for k in range(8)]
            if pend is not None:
                pm, prow, pval = pend
                for k in range(8):
                    pm[pl.ds(prow[k], 1), :] = pval[k]
            if j < 128:
                pend = (m, rows, vals)
                if j % 16 == 0 and hooks: hooks[j // 16]()
    def half(t, nxt, cur_u, nxt_u, cur_rs):
        cs = cols(nxt)
        hooks = [functools.partial(make_u, cs, k, nxt_u) for k in range(8)]
        rmw_half(cur_rs, cur_u, hooks)
    cs = cols(0)
    for k in range(8): make_u(cs, k, ua)
    NS = len(rss)
    for q in range(NS - 1): rows_copy(q, rss[q], q).start()
    def body(i, c):
        for q in range(NS):
            t = NS * i + q
            rows_copy(t, rss[q], q).wait()
            rows_copy(jnp.minimum(t + NS - 1, tiles - 1), rss[(q + NS - 1) % NS], (q + NS - 1) % NS).start()
            half(t, jnp.minimum(t + 1, tiles - 1), (ua, ub)[q % 2], (ub, ua)[q % 2], rss[q])
        return c
    lax.fori_loop(0, tiles // NS, body, 0)
    for q in range(NS - 1): rows_copy(tiles - 1, rss[q], q).wait()

    pos = lax.broadcasted_iota(jnp.int32, (8 * tiles, 128), 0) * 128 + lax.broadcasted_iota(jnp.int32, (8 * tiles, 128), 1)
    lane_row = lax.broadcasted_iota(jnp.int32, (1, 128), 1)
    def one_left(i, c):
        p = jnp.min(jnp.where(left_v[...] > 0.5, pos, 8 * tiles * 128).astype(F32)).astype(jnp.int32)
        here = pos == p
        left_v[...] = jnp.where(here, 0.0, left_v[...])
        pick = lambda x: jnp.sum(jnp.where(here, x, 0.0))
        dst = pick(dst_v[...].astype(F32)).astype(jnp.int32)
        row = ((dst >> 7) << 11) + pick(src_v[...].astype(F32)).astype(jnp.int32)
        ma[pl.ds(row, 1), :] = ma[pl.ds(row, 1), :] + jnp.where(lane_row == (dst & 127), pick(w_v[...]), 0.0)
        return c
    lax.fori_loop(0, n_left.astype(jnp.int32), one_left, 0)


def build(src,dst,w):
    n=src.shape[0]; nb=n//128
    s2=lambda a:pltpu.with_memory_space_constraint(a.reshape(nb,128), pltpu.HBM)
    o=jax.ShapeDtypeStruct((LAST+8,128),F32)
    V=pl.BlockSpec(memory_space=pltpu.VMEM); H=pl.BlockSpec(memory_space=pltpu.HBM)
    S=pltpu.VMEM
    return pl.pallas_call(build_kernel, out_shape=[o]*2, in_specs=[H]*3, out_specs=[V]*2,
        scratch_shapes=[S((nb,128),jnp.int32)]*2+[S((nb,128),F32)]+[S((nb,128),jnp.int32)]+[S((nb,128),F32)]*4
          +[S((8,128,128),F32)]*2+[pltpu.SMEM((8,128),jnp.int32)]*NSM+[pltpu.SemaphoreType.DMA((3,)),pltpu.SemaphoreType.DMA((NSM,))],
        name="build", cost_estimate=pl.CostEstimate(flops=10**10, bytes_accessed=80 * 10**6, transcendentals=0), compiler_params=pltpu.CompilerParams(vmem_limit_bytes=36*1024*1024))(s2(src),s2(dst),s2(w))


def step_kernel(
    x_ref, w1_ref, w2_ref, send_ref, ma_ref, mb_ref, lab_ref, mask_ref,
    out_ref, small_ref,
    s0_ref, s1_ref, sb1, hp1, hn1, sb2, hp2, hn2, gb2, ra2, rb2, gb1, ra1, rb1,
    y_ref, hid_ref, part, rc, a1, rx, cnt, cntr, sml, smlr, own_ref, dy_ref, w2p, bh_ref, bm_ref, bl_ref, r0_ref, r1_ref, ssem, rsem, fsem, frsem, gsem, grsem,
):
    me = lax.axis_index(AXIS)
    num = 128
    core = lax.rem(me, 2)
    cx = lax.rem(me // 2, 4)
    cy = lax.rem(me // 8, 4)
    cz = me // 32
    away = lax.rem(me + num - 1 + 2 * core, num)
    twin = me + 1 - 2 * core
    dims = ((cx, 2), (cy, 8), (cz, 32))

    def peer(dim, d):
        c, stride = dims[dim]
        p = lax.rem(c + d, 4)
        return p, me + (p - c) * stride

    barrier = pltpu.get_barrier_semaphore()
    targets = [away, twin] + [peer(k, d)[1] for k in range(3) for d in (1, 2, 3)]
    for t in targets:
        pl.semaphore_signal(barrier, inc=1, device_id=(t,), device_id_type=pl.DeviceIdType.MESH)

    counter = [0]

    def copy(src, dst, dev):
        k = counter[0]
        counter[0] += 1
        c = pltpu.make_async_remote_copy(
            src_ref=src, dst_ref=dst, send_sem=ssem.at[k], recv_sem=rsem.at[k],
            device_id=(dev,), device_id_type=pl.DeviceIdType.MESH,
        )
        c.start()
        return c

    cnt[...] = jnp.broadcast_to(jnp.sum(mask_ref[...].astype(F32), axis=1, keepdims=True), (8, 128))

    def small_start(val, recv, stage):
        if stage == 0:
            return [copy(val, recv.at[0, 0], twin)]
        c, _ = dims[stage - 1]
        recv[stage, c] = val[...]
        return [copy(val, recv.at[stage, c], peer(stage - 1, d)[1]) for d in (1, 2, 3)]

    def small_end(copies, val, recv, stage):
        for c in copies:
            c.wait()
        if stage == 0:
            val[...] = val[...] + recv[0, 0]
        else:
            val[...] = (recv[stage, 0] + recv[stage, 1]) + (recv[stage, 2] + recv[stage, 3])


    w2p[...] = jnp.zeros((HID, HID), F32)
    w2p[0:19, :] = w2_ref[...]
    w2t = w2p[0:PADC, :].astype(BF16)
    w2n = w2p[...].T.astype(BF16)[:, 0:PADC]

    node = lax.broadcasted_iota(jnp.int32, (NODES, HALO), 0)
    s0_ref[...] = jnp.where(node == send_ref[pl.ds(1 - core, 1), :], 1.0, 0.0).astype(BF16)
    s1_ref[...] = jnp.where(node == send_ref[pl.ds(core, 1), :], 1.0, 0.0).astype(BF16)

    t1 = dot_n(x_ref[...], w1_ref[...].astype(BF16))
    t1 = t1.T.astype(BF16)
    sb1[1] = dot_n(t1, s1_ref[...]).astype(BF16)
    pl.semaphore_wait(barrier, len(targets))
    c_p = copy(sb1.at[1], hp1, away)
    sb1[0] = dot_n(t1, s0_ref[...]).astype(BF16)
    c_n = copy(sb1.at[0], hn1, twin)
    cc = small_start(cnt, cntr, 0)

    def agg(e, lo, hi):
        acc = dot_n(e, bl_ref[lo:hi, :])
        acc = acc + dot_n(e, bm_ref[lo:hi, :])
        return acc + dot_n(e, bh_ref[lo:hi, :])

    def split_block(first, source, blocks):
        def one(i, c):
            rows = pl.ds(pl.multiple_of((first + i) * 128, 128), 128)
            for j in range(NODES // 128):
                from_rows = pl.ds(pl.multiple_of(j * EXT + (source + i) * 128, 128), 128)
                h, m, l = split3(ma_ref[from_rows, :] + mb_ref[from_rows, :])
                cols = pl.ds(j * 128, 128)
                bh_ref[rows, cols] = h
                bm_ref[rows, cols] = m
                bl_ref[rows, cols] = l
            return c

        lax.fori_loop(0, blocks, one, 0)

    split_block(0, 0, 8)
    y_ref[...] = agg(t1, 0, NODES)
    split_block(12, 12 - 4 * core, 4)
    split_block(8, 8 + 4 * core, 4)
    column = lax.broadcasted_iota(jnp.int32, (HALO, NODES), 1).astype(F32)
    for k, r_ref in ((1 - core, r0_ref), (core, r1_ref)):
        ids = jnp.broadcast_to(send_ref[pl.ds(k, 1), :].astype(F32), (8, HALO)).T[:, 0:1]
        r_ref[...] = jnp.where(column == ids, 1.0, 0.0).astype(BF16)
    small_end(cc, cnt, cntr, 0)
    cc = small_start(cnt, cntr, 1)
    c_n.wait()
    y_ref[...] += agg(hn1[...], NODES + HALO, EXT)
    c_p.wait()
    y = y_ref[...] + agg(hp1[...], NODES, NODES + HALO)
    y_ref[...] = y
    small_end(cc, cnt, cntr, 1)
    cc = small_start(cnt, cntr, 2)
    hid = jnp.maximum(y, 0.0).astype(BF16)
    hid_ref[...] = hid
    t2 = dot_n(w2t, hid).astype(BF16)
    sb2[1] = dot_n(t2, s1_ref[...]).astype(BF16)
    c_p = copy(sb2.at[1], hp2, away)
    sb2[0] = dot_n(t2, s0_ref[...]).astype(BF16)
    c_n = copy(sb2.at[0], hn2, twin)
    z = agg(t2, 0, NODES)
    small_end(cc, cnt, cntr, 2)
    cc = small_start(cnt, cntr, 3)
    c_n.wait()
    z = z + agg(hn2[...], NODES + HALO, EXT)
    c_p.wait()
    z = z + agg(hp2[...], NODES, NODES + HALO)
    small_end(cc, cnt, cntr, 3)
    count = jnp.maximum(cnt[0:1, 0:1], 1.0)

    cls = lax.broadcasted_iota(jnp.int32, (PADC, NODES), 0)
    real = cls < 19
    mask = mask_ref[...].astype(F32)
    zm = jnp.where(real, z, -jnp.inf)
    top = jnp.max(zm, axis=0, keepdims=True)
    norm = jnp.log(jnp.sum(jnp.where(real, jnp.exp(z - top), 0.0), axis=0, keepdims=True)) + top
    hot = (cls == lab_ref[...]).astype(F32)
    picked = jnp.sum(z * hot, axis=0, keepdims=True)
    loss = jnp.sum(mask * (norm - picked), axis=1, keepdims=True)
    dz = (jnp.where(real, jnp.exp(z - norm), 0.0) - hot) * (mask / count)

    def agg_back(d, lo, hi):
        n = d.shape[0]
        dh, dm, dl = split3(d)
        rh = dot_t(jnp.concatenate([dh, dm, dl], axis=0), bh_ref[lo:hi, :])
        rm = dot_t(jnp.concatenate([dh, dm], axis=0), bm_ref[lo:hi, :])
        rl = dot_t(dh, bl_ref[lo:hi, :])
        return rh[0:n] + ((rh[n:2 * n] + rm[0:n]) + (rh[2 * n:3 * n] + (rm[n:2 * n] + rl)))

    def returned(r, s_rows):
        n = r.shape[0]
        t = dot_n(jnp.concatenate(split3(r), axis=0), s_rows)
        return t[0:n] + (t[n:2 * n] + t[2 * n:3 * n])

    gb2[0] = agg_back(dz, NODES, NODES + HALO)
    c_p = copy(gb2.at[0], ra2, away)
    gb2[1] = agg_back(dz, NODES + HALO, EXT)
    c_n = copy(gb2.at[1], rb2, twin)
    own = agg_back(dz, 0, NODES)
    c_n.wait()
    own = own + returned(rb2[...], r0_ref[...])
    c_p.wait()
    dt2 = (own + returned(ra2[...], r1_ref[...])).astype(BF16)
    g2 = dot_t(dt2, hid_ref[...])
    sml[...] = g2
    sml[24:32, :] = jnp.broadcast_to(loss, (8, 128))
    cs = small_start(sml, smlr, 0)
    dh = dot_n(w2n, dt2)
    dy_ref[...] = jnp.where(y_ref[...] > 0.0, dh, 0.0)
    back = []
    for side, land, dev in ((0, ra1, away), (1, rb1, twin)):
        for h in range(2):
            first = NODES + side * HALO + h * QTR
            gb1[side, h] = agg_back(dy_ref[...], first, first + QTR)
            back.append(copy(gb1.at[side, h], land.at[h], dev))
    small_end(cs, sml, smlr, 0)
    cs = small_start(sml, smlr, 1)
    own_ref[...] = agg_back(dy_ref[...], 0, NODES)
    small_end(cs, sml, smlr, 1)
    cs = small_start(sml, smlr, 2)
    for side, land, rows_ref in ((1, rb1, r0_ref), (0, ra1, r1_ref)):
        for h in range(2):
            back[2 * side + h].wait()
            own_ref[...] += returned(land[h], rows_ref[pl.ds(h * QTR, QTR), :])
    dt1 = own_ref[...].astype(BF16)

    mine = pl.ds(pl.multiple_of(core * 512, 512), 512)
    other = pl.ds(pl.multiple_of((1 - core) * 512, 512), 512)
    part[...] = dot_n(dt1, x_ref[:, other]).T
    swap = copy(part, rc, twin)
    small_end(cs, sml, smlr, 2)
    cs = small_start(sml, smlr, 3)
    own_half = dot_n(dt1, x_ref[:, mine]).T
    swap.wait()
    a1[...] = own_half + rc[...]

    chip = me // 2

    def rows_of(q):
        return pl.ds(pl.multiple_of(q * 8, 8), 8)

    spot = lax.rem(chip, 16)
    mine8 = pl.ds(pl.multiple_of(core * 512 + chip * 8, 8), 8)
    shifts = [(dz, dr) for dz in (2, 1, 3, 0) for dr in range(16) if dz + dr > 0]

    def far(dz, dr):
        q = lax.rem(cz + dz, 4) * 16 + lax.rem(spot + dr, 16)
        return dz * 16 + dr - 1, q, q * 2 + core

    def far_copy(dz, dr, gather):
        k, q, dev = far(dz, dr)
        src = out_ref.at[mine8] if gather else a1.at[rows_of(q)]
        return pltpu.make_async_remote_copy(
            src_ref=src, dst_ref=src if gather else rx.at[k],
            send_sem=(gsem if gather else fsem).at[k], recv_sem=(grsem if gather else frsem).at[k],
            device_id=(dev,), device_id_type=pl.DeviceIdType.MESH,
        )

    scatters = [far_copy(dz, dr, False) for dz, dr in shifts]
    for c in scatters:
        c.start()
    small_end(cs, sml, smlr, 3)
    for c in scatters:
        c.wait()
    total = [a1[rows_of(chip), :]] + [rx[k] for k in range(CHIPS - 1)]
    while len(total) > 1:
        total = [total[k] + total[k + 1] for k in range(0, len(total), 2)]
    out_ref[mine8, :] = total[0]
    gathers = {(dz, dr): far_copy(dz, dr, True) for dz, dr in shifts}
    for c in gathers.values():
        c.start()
    last = []
    for dz in (0, 1, 3, 2):
        for dr in range(16):
            if dz + dr > 0:
                gathers[dz, dr].wait()
        plane = pl.ds(pl.multiple_of(core * 512 + lax.rem(cz - dz + 4, 4) * 128, 128), 128)
        last.append(copy(out_ref.at[plane], out_ref.at[plane], twin))
    small_ref[...] = sml[...]
    small_ref[24:32, :] = sml[24:32, :] / count
    for c in last:
        c.wait()


def finish_kernel(one_in, small_in, loss_ref, one_ref, two_ref, two_v, sem):
    one = pltpu.make_async_copy(one_in, one_ref, sem.at[0])
    one.start()
    two_v[...] = small_in[0:19, :]
    two = pltpu.make_async_copy(two_v, two_ref, sem.at[1])
    two.start()
    loss_ref[0, 0] = jnp.max(small_in[24:25, :])
    one.wait()
    two.wait()


def finish(one, small):
    vmem = pl.BlockSpec(memory_space=pltpu.VMEM)
    hbm = pl.BlockSpec(memory_space=pltpu.HBM)
    return pl.pallas_call(
        finish_kernel,
        out_shape=[
            jax.ShapeDtypeStruct((1, 1), F32), jax.ShapeDtypeStruct(one.shape, F32), jax.ShapeDtypeStruct((19, HID), F32),
        ],
        in_specs=[vmem] * 2,
        out_specs=[pl.BlockSpec(memory_space=pltpu.SMEM), hbm, hbm],
        scratch_shapes=[pltpu.VMEM((19, HID), F32), pltpu.SemaphoreType.DMA((2,))],
        name="finish",
        compiler_params=pltpu.CompilerParams(vmem_limit_bytes=4 * 1024 * 1024),
    )(one, small)


def step(x, w_one, w_two, send_rows, src, dst, w, labels, mask):
    ma, mb = build(src, dst, w)
    vmem = pl.BlockSpec(memory_space=pltpu.VMEM)
    n_sem = 36
    V = pltpu.VMEM
    one, small = pl.pallas_call(
        step_kernel,
        out_shape=[
            jax.ShapeDtypeStruct((1024, HID), F32),
            jax.ShapeDtypeStruct((PADC, HID), F32),
        ],
        in_specs=[vmem] * 8,
        out_specs=[vmem] * 2,
        scratch_shapes=[
            V((NODES, HALO), BF16), V((NODES, HALO), BF16),
            V((2, HID, HALO), BF16), V((HID, HALO), BF16), V((HID, HALO), BF16),
            V((2, PADC, HALO), BF16), V((PADC, HALO), BF16), V((PADC, HALO), BF16),
            V((2, PADC, HALO), F32), V((PADC, HALO), F32), V((PADC, HALO), F32),
            V((2, 2, HID, QTR), F32), V((2, HID, QTR), F32), V((2, HID, QTR), F32),
            V((HID, NODES), F32), V((HID, NODES), BF16),
            V((512, HID), F32), V((512, HID), F32), V((512, HID), F32),
            V((CHIPS - 1, 8, HID), F32),
            V((8, 128), F32), V((4, 4, 8, 128), F32), V((PADC, 128), F32), V((4, 4, PADC, 128), F32),
            V((HID, NODES), F32), V((HID, NODES), F32), V((HID, HID), F32),
            V((EXT, NODES), BF16), V((EXT, NODES), BF16), V((EXT, NODES), BF16),
            V((HALO, NODES), BF16), V((HALO, NODES), BF16),
            pltpu.SemaphoreType.DMA((n_sem,)), pltpu.SemaphoreType.DMA((n_sem,)),
            *[pltpu.SemaphoreType.DMA((CHIPS - 1,))] * 4,
        ],
        name="step",
        compiler_params=pltpu.CompilerParams(
            collective_id=0, has_side_effects=True, vmem_limit_bytes=31 * 1024 * 1024
        ),
    )(x, w_one, w_two.T, send_rows, ma, mb, labels.reshape(1, NODES), mask.reshape(1, NODES))
    loss, one, two = finish(one, small)
    return loss.reshape(()), one, two.T


def solution(mesh):
    row = P(AXIS)
    return jax.shard_map(
        step, mesh=mesh, in_specs=(row, P(), P(), row, row, row, row, row, row),
        out_specs=(P(), P(), P()), check_vma=False,
    )
```

```python
import functools

import jax
import jax.numpy as jnp
from jax import lax
from jax.experimental import pallas as pl
from jax.experimental.pallas import tpu as pltpu
from jax.sharding import PartitionSpec as P

AXIS = "graph"
F32 = jnp.float32
BF16 = jnp.bfloat16
NODES = 1024
HALO = 512
QTR = HALO // 2
EXT = NODES + 2 * HALO
HID = 128
PADC = 32
LAST = 8 * EXT
NSM = 4
CHIPS = 64
ROW_N = (((1,), (0,)), ((), ()))
ROW_T = (((1,), (1,)), ((), ()))


def split3(x):
    high = x.astype(BF16)
    rest = x - high.astype(F32)
    mid = rest.astype(BF16)
    low = (rest - mid.astype(F32)).astype(BF16)
    return high, mid, low


def dot_n(a, b):
    return lax.dot_general(a, b, ROW_N, preferred_element_type=F32)


def dot_t(a, b):
    return lax.dot_general(a, b, ROW_T, preferred_element_type=F32)


def build_kernel(src_hbm, dst_hbm, w_hbm, ma, mb, src_v, dst_v, w_v, row_v, lane_v, lane2_v, w2_v, left_v, ua, ub, *rest):
    rss, sem, rsem = rest[:NSM], rest[NSM], rest[NSM + 1]
    tiles = src_v.shape[0] // 8
    loads = [pltpu.make_async_copy(a, b, sem.at[k]) for k, (a, b) in enumerate(((src_hbm, src_v), (dst_hbm, dst_v), (w_hbm, w_v)))]
    for c in loads: c.start()
    def zero(i, c):
        z = jnp.zeros((256, 128), F32)
        rows = pl.ds(pl.multiple_of(i * 256, 256), 256)
        ma[rows, :] = z; mb[rows, :] = z
        return c
    lax.fori_loop(0, LAST // 256, zero, 0)
    for c in loads: c.wait()
    sub = lax.broadcasted_iota(jnp.int32, (8, 128), 0)
    def prep(t, left):
        tile = pl.ds(pl.multiple_of(t * 8, 8), 8)
        dst = dst_v[tile, :]
        row = ((dst >> 7) << 11) + src_v[tile, :]
        lane = (dst & 127).astype(F32)
        w = w_v[tile, :]
        seen = jnp.zeros((8, 128), F32); lane2 = seen; w2 = seen
        for d in range(1, 8):
            same = jnp.logical_and(row == pltpu.roll(row, d, axis=0), sub >= d)
            seen = seen + jnp.where(same, 1.0, 0.0)
            lane2 = lane2 + jnp.where(same, pltpu.roll(lane, d, axis=0), 0.0)
            w2 = w2 + jnp.where(same, pltpu.roll(w, d, axis=0), 0.0)
        late = seen > 1.5
        row_v[tile, :] = jnp.where(late, LAST, row)
        lane_v[tile, :] = lane
        lane2_v[tile, :] = lane2
        w2_v[tile, :] = w2
        mark = jnp.where(late, 1.0, 0.0)
        left_v[tile, :] = mark
        return left + mark
    left = lax.fori_loop(0, tiles, prep, jnp.zeros((8, 128), F32))
    n_left = jnp.sum(left)

    def rows_copy(t, rs, k):
        return pltpu.make_async_copy(row_v.at[pl.ds(pl.multiple_of(t * 8, 8), 8), :], rs, rsem.at[k])
    lanes = lax.broadcasted_iota(jnp.int32, (128, 128), 1).astype(F32)
    def cols(t):
        tile = pl.ds(pl.multiple_of(t * 8, 8), 8)
        return [r[tile, :].T for r in (lane_v, w_v, lane2_v, w2_v)]
    def make_u(cs, k, u):
        l1, w1, l2, w2 = [jnp.broadcast_to(c[:, k:k + 1], (128, 128)) for c in cs]
        u[k] = jnp.where(lanes == l1, w1, 0.0) + jnp.where(lanes == l2, w2, 0.0)
    def rmw_half(rs, u, hooks):
        pend = None
        for j in range(129):
            if j < 128:
                m = ma if j % 2 == 0 else mb
                rows = [rs[k, j] for k in range(8)]
                vals = [m[pl.ds(rows[k], 1), :] + u[k, pl.ds(j, 1), :] for k in range(8)]
            if pend is not None:
                pm, prow, pval = pend
                for k in range(8):
                    pm[pl.ds(prow[k], 1), :] = pval[k]
            if j < 128:
                pend = (m, rows, vals)
                if j % 16 == 0 and hooks: hooks[j // 16]()
    def half(t, nxt, cur_u, nxt_u, cur_rs):
        cs = cols(nxt)
        hooks = [functools.partial(make_u, cs, k, nxt_u) for k in range(8)]
        rmw_half(cur_rs, cur_u, hooks)
    cs = cols(0)
    for k in range(8): make_u(cs, k, ua)
    NS = len(rss)
    for q in range(NS - 1): rows_copy(q, rss[q], q).start()
    def body(i, c):
        for q in range(NS):
            t = NS * i + q
            rows_copy(t, rss[q], q).wait()
            rows_copy(jnp.minimum(t + NS - 1, tiles - 1), rss[(q + NS - 1) % NS], (q + NS - 1) % NS).start()
            half(t, jnp.minimum(t + 1, tiles - 1), (ua, ub)[q % 2], (ub, ua)[q % 2], rss[q])
        return c
    lax.fori_loop(0, tiles // NS, body, 0)
    for q in range(NS - 1): rows_copy(tiles - 1, rss[q], q).wait()

    pos = lax.broadcasted_iota(jnp.int32, (8 * tiles, 128), 0) * 128 + lax.broadcasted_iota(jnp.int32, (8 * tiles, 128), 1)
    lane_row = lax.broadcasted_iota(jnp.int32, (1, 128), 1)
    def one_left(i, c):
        p = jnp.min(jnp.where(left_v[...] > 0.5, pos, 8 * tiles * 128).astype(F32)).astype(jnp.int32)
        here = pos == p
        left_v[...] = jnp.where(here, 0.0, left_v[...])
        pick = lambda x: jnp.sum(jnp.where(here, x, 0.0))
        dst = pick(dst_v[...].astype(F32)).astype(jnp.int32)
        row = ((dst >> 7) << 11) + pick(src_v[...].astype(F32)).astype(jnp.int32)
        ma[pl.ds(row, 1), :] = ma[pl.ds(row, 1), :] + jnp.where(lane_row == (dst & 127), pick(w_v[...]), 0.0)
        return c
    lax.fori_loop(0, n_left.astype(jnp.int32), one_left, 0)


def build(src,dst,w):
    n=src.shape[0]; nb=n//128
    s2=lambda a:pltpu.with_memory_space_constraint(a.reshape(nb,128), pltpu.HBM)
    o=jax.ShapeDtypeStruct((LAST+8,128),F32)
    V=pl.BlockSpec(memory_space=pltpu.VMEM); H=pl.BlockSpec(memory_space=pltpu.HBM)
    S=pltpu.VMEM
    return pl.pallas_call(build_kernel, out_shape=[o]*2, in_specs=[H]*3, out_specs=[V]*2,
        scratch_shapes=[S((nb,128),jnp.int32)]*2+[S((nb,128),F32)]+[S((nb,128),jnp.int32)]+[S((nb,128),F32)]*4
          +[S((8,128,128),F32)]*2+[pltpu.SMEM((8,128),jnp.int32)]*NSM+[pltpu.SemaphoreType.DMA((3,)),pltpu.SemaphoreType.DMA((NSM,))],
        name="build", cost_estimate=pl.CostEstimate(flops=10**10, bytes_accessed=80 * 10**6, transcendentals=0), compiler_params=pltpu.CompilerParams(vmem_limit_bytes=36*1024*1024))(s2(src),s2(dst),s2(w))


def step_kernel(
    x_ref, w1_ref, w2_ref, send_ref, ma_ref, mb_ref, lab_ref, mask_ref,
    out_ref, small_ref,
    s0_ref, s1_ref, sb1, hp1, hn1, sb2, hp2, hn2, ga2, gb2, ra2, rb2, gb1, ra1, rb1,
    y_ref, hid_ref, part, rc, a1, rx, cnt, cntr, sml, smlr, own_ref, dy_ref, w2p, bh_ref, bm_ref, bl_ref, r0_ref, r1_ref, ssem, rsem, fsem, frsem, gsem, grsem, bsem, brsem,
):
    me = lax.axis_index(AXIS)
    num = 128
    core = lax.rem(me, 2)
    cx = lax.rem(me // 2, 4)
    cy = lax.rem(me // 8, 4)
    cz = me // 32
    away = lax.rem(me + num - 1 + 2 * core, num)
    twin = me + 1 - 2 * core
    dims = ((cx, 2), (cy, 8), (cz, 32))

    def peer(dim, d):
        c, stride = dims[dim]
        p = lax.rem(c + d, 4)
        return p, me + (p - c) * stride

    barrier = pltpu.get_barrier_semaphore()
    targets = [away, twin] + [peer(k, d)[1] for k in range(3) for d in (1, 2, 3)]
    for t in targets:
        pl.semaphore_signal(barrier, inc=1, device_id=(t,), device_id_type=pl.DeviceIdType.MESH)

    counter = [0]

    def copy(src, dst, dev):
        k = counter[0]
        counter[0] += 1
        c = pltpu.make_async_remote_copy(
            src_ref=src, dst_ref=dst, send_sem=ssem.at[k], recv_sem=rsem.at[k],
            device_id=(dev,), device_id_type=pl.DeviceIdType.MESH,
        )
        c.start()
        return c

    cnt[...] = jnp.broadcast_to(jnp.sum(mask_ref[...].astype(F32), axis=1, keepdims=True), (8, 128))

    def small_start(val, recv, stage):
        if stage == 0:
            return [copy(val, recv.at[0, 0], twin)]
        c, _ = dims[stage - 1]
        recv[stage, c] = val[...]
        return [copy(val, recv.at[stage, c], peer(stage - 1, d)[1]) for d in (1, 2, 3)]

    def small_end(copies, val, recv, stage):
        for c in copies:
            c.wait()
        if stage == 0:
            val[...] = val[...] + recv[0, 0]
        else:
            val[...] = (recv[stage, 0] + recv[stage, 1]) + (recv[stage, 2] + recv[stage, 3])


    w2p[...] = jnp.zeros((HID, HID), F32)
    w2p[0:19, :] = w2_ref[...]
    w2t = w2p[0:PADC, :].astype(BF16)
    w2n = w2p[...].T.astype(BF16)[:, 0:PADC]

    node = lax.broadcasted_iota(jnp.int32, (NODES, HALO), 0)
    s0_ref[...] = jnp.where(node == send_ref[pl.ds(1 - core, 1), :], 1.0, 0.0).astype(BF16)
    s1_ref[...] = jnp.where(node == send_ref[pl.ds(core, 1), :], 1.0, 0.0).astype(BF16)

    t1 = dot_n(x_ref[...], w1_ref[...].astype(BF16))
    t1 = t1.T.astype(BF16)
    sb1[1] = dot_n(t1, s1_ref[...]).astype(BF16)
    pl.semaphore_wait(barrier, len(targets))
    c_p = copy(sb1.at[1], hp1, away)
    sb1[0] = dot_n(t1, s0_ref[...]).astype(BF16)
    c_n = copy(sb1.at[0], hn1, twin)
    cc = small_start(cnt, cntr, 0)

    def agg(e, lo, hi):
        acc = dot_n(e, bl_ref[lo:hi, :])
        acc = acc + dot_n(e, bm_ref[lo:hi, :])
        return acc + dot_n(e, bh_ref[lo:hi, :])

    def split_block(first, source, blocks):
        def one(i, c):
            rows = pl.ds(pl.multiple_of((first + i) * 128, 128), 128)
            for j in range(NODES // 128):
                from_rows = pl.ds(pl.multiple_of(j * EXT + (source + i) * 128, 128), 128)
                h, m, l = split3(ma_ref[from_rows, :] + mb_ref[from_rows, :])
                cols = pl.ds(j * 128, 128)
                bh_ref[rows, cols] = h
                bm_ref[rows, cols] = m
                bl_ref[rows, cols] = l
            return c

        lax.fori_loop(0, blocks, one, 0)

    split_block(0, 0, 8)
    y_ref[...] = agg(t1, 0, NODES)
    split_block(12, 12 - 4 * core, 4)
    split_block(8, 8 + 4 * core, 4)
    column = lax.broadcasted_iota(jnp.int32, (HALO, NODES), 1).astype(F32)
    for k, r_ref in ((1 - core, r0_ref), (core, r1_ref)):
        ids = jnp.broadcast_to(send_ref[pl.ds(k, 1), :].astype(F32), (8, HALO)).T[:, 0:1]
        r_ref[...] = jnp.where(column == ids, 1.0, 0.0).astype(BF16)
    small_end(cc, cnt, cntr, 0)
    cc = small_start(cnt, cntr, 1)
    c_n.wait()
    y_ref[...] += agg(hn1[...], NODES + HALO, EXT)
    c_p.wait()
    y = y_ref[...] + agg(hp1[...], NODES, NODES + HALO)
    y_ref[...] = y
    small_end(cc, cnt, cntr, 1)
    cc = small_start(cnt, cntr, 2)
    hid = jnp.maximum(y, 0.0).astype(BF16)
    hid_ref[...] = hid
    t2 = dot_n(w2t, hid).astype(BF16)
    sb2[1] = dot_n(t2, s1_ref[...]).astype(BF16)
    c_p = copy(sb2.at[1], hp2, away)
    sb2[0] = dot_n(t2, s0_ref[...]).astype(BF16)
    c_n = copy(sb2.at[0], hn2, twin)
    z = agg(t2, 0, NODES)
    small_end(cc, cnt, cntr, 2)
    cc = small_start(cnt, cntr, 3)
    c_n.wait()
    z = z + agg(hn2[...], NODES + HALO, EXT)
    c_p.wait()
    z = z + agg(hp2[...], NODES, NODES + HALO)
    small_end(cc, cnt, cntr, 3)
    count = jnp.maximum(cnt[0:1, 0:1], 1.0)

    cls = lax.broadcasted_iota(jnp.int32, (PADC, NODES), 0)
    real = cls < 19
    mask = mask_ref[...].astype(F32)
    zm = jnp.where(real, z, -jnp.inf)
    top = jnp.max(zm, axis=0, keepdims=True)
    norm = jnp.log(jnp.sum(jnp.where(real, jnp.exp(z - top), 0.0), axis=0, keepdims=True)) + top
    hot = (cls == lab_ref[...]).astype(F32)
    picked = jnp.sum(z * hot, axis=0, keepdims=True)
    loss = jnp.sum(mask * (norm - picked), axis=1, keepdims=True)
    dz = (jnp.where(real, jnp.exp(z - norm), 0.0) - hot) * (mask / count)

    def agg_back(d, lo, hi):
        n = d.shape[0]
        dh, dm, dl = split3(d)
        rh = dot_t(jnp.concatenate([dh, dm, dl], axis=0), bh_ref[lo:hi, :])
        rm = dot_t(jnp.concatenate([dh, dm], axis=0), bm_ref[lo:hi, :])
        rl = dot_t(dh, bl_ref[lo:hi, :])
        return rh[0:n] + ((rh[n:2 * n] + rm[0:n]) + (rh[2 * n:3 * n] + (rm[n:2 * n] + rl)))

    def returned(r, s_rows):
        n = r.shape[0]
        t = dot_n(jnp.concatenate(split3(r), axis=0), s_rows)
        return t[0:n] + (t[n:2 * n] + t[2 * n:3 * n])

    c_p = []
    for h in range(2):
        ga2[h] = agg_back(dz, NODES + h * QTR, NODES + (h + 1) * QTR)
        c_p.append(copy(ga2.at[h], ra2.at[h], away))
    gb2[...] = agg_back(dz, NODES + HALO, EXT)
    c_n = copy(gb2, rb2, twin)
    own = agg_back(dz, 0, NODES)
    c_n.wait()
    own = own + returned(rb2[...], r0_ref[...])
    for h in range(2):
        c_p[h].wait()
        own = own + returned(ra2[h], r1_ref[pl.ds(h * QTR, QTR), :])
    dt2 = own.astype(BF16)
    g2 = dot_t(dt2, hid_ref[...])
    sml[...] = g2
    sml[24:32, :] = jnp.broadcast_to(loss, (8, 128))
    cs = small_start(sml, smlr, 0)
    dh = dot_n(w2n, dt2)
    dy_ref[...] = jnp.where(y_ref[...] > 0.0, dh, 0.0)
    back = []
    for side, land, dev in ((0, ra1, away), (1, rb1, twin)):
        for h in range(2):
            first = NODES + side * HALO + h * QTR
            gb1[side, h] = agg_back(dy_ref[...], first, first + QTR)
            back.append(copy(gb1.at[side, h], land.at[h], dev))
    small_end(cs, sml, smlr, 0)
    cs = small_start(sml, smlr, 1)
    own_ref[...] = agg_back(dy_ref[...], 0, NODES)
    small_end(cs, sml, smlr, 1)
    cs = small_start(sml, smlr, 2)
    for side, land, rows_ref in ((1, rb1, r0_ref), (0, ra1, r1_ref)):
        for h in range(2):
            back[2 * side + h].wait()
            own_ref[...] += returned(land[h], rows_ref[pl.ds(h * QTR, QTR), :])
    dt1 = own_ref[...].astype(BF16)

    mine = pl.ds(pl.multiple_of(core * 512, 512), 512)
    other = pl.ds(pl.multiple_of((1 - core) * 512, 512), 512)
    part[...] = dot_n(dt1, x_ref[:, other]).T
    swap = copy(part, rc, twin)
    small_end(cs, sml, smlr, 2)
    cs = small_start(sml, smlr, 3)
    own_half = dot_n(dt1, x_ref[:, mine]).T
    swap.wait()
    a1[...] = own_half + rc[...]

    chip = me // 2

    def rows_of(q):
        return pl.ds(pl.multiple_of(q * 8, 8), 8)

    spot = lax.rem(chip, 16)
    mine8 = pl.ds(pl.multiple_of(core * 512 + chip * 8, 8), 8)
    shifts = [(dz, dr) for dz in (2, 1, 3, 0) for dr in range(16) if dz + dr > 0]

    def far(dz, dr):
        q = lax.rem(cz + dz, 4) * 16 + lax.rem(spot + dr, 16)
        return dz * 16 + dr - 1, q, q * 2 + core

    def far_copy(dz, dr, gather):
        k, q, dev = far(dz, dr)
        src = out_ref.at[mine8] if gather else a1.at[rows_of(q)]
        return pltpu.make_async_remote_copy(
            src_ref=src, dst_ref=src if gather else rx.at[k],
            send_sem=(gsem if gather else fsem).at[k], recv_sem=(grsem if gather else frsem).at[k],
            device_id=(dev,), device_id_type=pl.DeviceIdType.MESH,
        )

    scatters = [far_copy(dz, dr, False) for dz, dr in shifts]
    for c in scatters:
        c.start()
    small_end(cs, sml, smlr, 3)
    for c in scatters:
        c.wait()
    total = [a1[rows_of(chip), :]] + [rx[k] for k in range(CHIPS - 1)]
    while len(total) > 1:
        total = [total[k] + total[k + 1] for k in range(0, len(total), 2)]
    out_ref[mine8, :] = total[0]
    gathers = {(dz, dr): far_copy(dz, dr, True) for dz, dr in shifts}
    both = []
    for dr in range(16):
        _, q, _ = far(2, dr)
        both.append(pltpu.make_async_remote_copy(
            src_ref=out_ref.at[mine8], dst_ref=out_ref.at[mine8], send_sem=bsem.at[dr], recv_sem=brsem.at[dr],
            device_id=(q * 2 + 1 - core,), device_id_type=pl.DeviceIdType.MESH,
        ))
    for c in [gathers[2, dr] for dr in range(16)] + both + [c for (dz, _), c in gathers.items() if dz != 2]:
        c.start()
    last = []
    for dz in (0, 1, 3, 2):
        for dr in range(16):
            if dz + dr > 0:
                gathers[dz, dr].wait()
        if dz == 2:
            continue
        plane = pl.ds(pl.multiple_of(core * 512 + lax.rem(cz - dz + 4, 4) * 128, 128), 128)
        last.append(copy(out_ref.at[plane], out_ref.at[plane], twin))
    small_ref[...] = sml[...]
    small_ref[24:32, :] = sml[24:32, :] / count
    for c in both + last:
        c.wait()


def finish_kernel(one_in, small_in, loss_ref, one_ref, two_ref, two_v, sem):
    one = pltpu.make_async_copy(one_in, one_ref, sem.at[0])
    one.start()
    two_v[...] = small_in[0:19, :]
    two = pltpu.make_async_copy(two_v, two_ref, sem.at[1])
    two.start()
    loss_ref[0, 0] = jnp.max(small_in[24:25, :])
    one.wait()
    two.wait()


def finish(one, small):
    vmem = pl.BlockSpec(memory_space=pltpu.VMEM)
    hbm = pl.BlockSpec(memory_space=pltpu.HBM)
    return pl.pallas_call(
        finish_kernel,
        out_shape=[
            jax.ShapeDtypeStruct((1, 1), F32), jax.ShapeDtypeStruct(one.shape, F32), jax.ShapeDtypeStruct((19, HID), F32),
        ],
        in_specs=[vmem] * 2,
        out_specs=[pl.BlockSpec(memory_space=pltpu.SMEM), hbm, hbm],
        scratch_shapes=[pltpu.VMEM((19, HID), F32), pltpu.SemaphoreType.DMA((2,))],
        name="finish",
        compiler_params=pltpu.CompilerParams(vmem_limit_bytes=4 * 1024 * 1024),
    )(one, small)


def step(x, w_one, w_two, send_rows, src, dst, w, labels, mask):
    ma, mb = build(src, dst, w)
    vmem = pl.BlockSpec(memory_space=pltpu.VMEM)
    n_sem = 36
    V = pltpu.VMEM
    one, small = pl.pallas_call(
        step_kernel,
        out_shape=[
            jax.ShapeDtypeStruct((1024, HID), F32),
            jax.ShapeDtypeStruct((PADC, HID), F32),
        ],
        in_specs=[vmem] * 8,
        out_specs=[vmem] * 2,
        scratch_shapes=[
            V((NODES, HALO), BF16), V((NODES, HALO), BF16),
            V((2, HID, HALO), BF16), V((HID, HALO), BF16), V((HID, HALO), BF16),
            V((2, PADC, HALO), BF16), V((PADC, HALO), BF16), V((PADC, HALO), BF16),
            V((2, PADC, QTR), F32), V((PADC, HALO), F32), V((2, PADC, QTR), F32), V((PADC, HALO), F32),
            V((2, 2, HID, QTR), F32), V((2, HID, QTR), F32), V((2, HID, QTR), F32),
            V((HID, NODES), F32), V((HID, NODES), BF16),
            V((512, HID), F32), V((512, HID), F32), V((512, HID), F32),
            V((CHIPS - 1, 8, HID), F32),
            V((8, 128), F32), V((4, 4, 8, 128), F32), V((PADC, 128), F32), V((4, 4, PADC, 128), F32),
            V((HID, NODES), F32), V((HID, NODES), F32), V((HID, HID), F32),
            V((EXT, NODES), BF16), V((EXT, NODES), BF16), V((EXT, NODES), BF16),
            V((HALO, NODES), BF16), V((HALO, NODES), BF16),
            pltpu.SemaphoreType.DMA((n_sem,)), pltpu.SemaphoreType.DMA((n_sem,)),
            *[pltpu.SemaphoreType.DMA((CHIPS - 1,))] * 4,
            *[pltpu.SemaphoreType.DMA((16,))] * 2,
        ],
        name="step",
        compiler_params=pltpu.CompilerParams(
            collective_id=0, has_side_effects=True, vmem_limit_bytes=31 * 1024 * 1024
        ),
    )(x, w_one, w_two.T, send_rows, ma, mb, labels.reshape(1, NODES), mask.reshape(1, NODES))
    loss, one, two = finish(one, small)
    return loss.reshape(()), one, two.T


def solution(mesh):
    row = P(AXIS)
    return jax.shard_map(
        step, mesh=mesh, in_specs=(row, P(), P(), row, row, row, row, row, row),
        out_specs=(P(), P(), P()), check_vma=False,
    )
```

```python
import functools

import jax
import jax.numpy as jnp
from jax import lax
from jax.experimental import pallas as pl
from jax.experimental.pallas import tpu as pltpu
from jax.sharding import PartitionSpec as P

AXIS = "graph"
F32 = jnp.float32
BF16 = jnp.bfloat16
NODES = 1024
HALO = 512
QTR = HALO // 2
EXT = NODES + 2 * HALO
HID = 128
PADC = 32
LAST = 8 * EXT
NSM = 4
CHIPS = 64
ROW_N = (((1,), (0,)), ((), ()))
ROW_T = (((1,), (1,)), ((), ()))


def split3(x):
    high = x.astype(BF16)
    rest = x - high.astype(F32)
    mid = rest.astype(BF16)
    low = (rest - mid.astype(F32)).astype(BF16)
    return high, mid, low


def dot_n(a, b):
    return lax.dot_general(a, b, ROW_N, preferred_element_type=F32)


def dot_t(a, b):
    return lax.dot_general(a, b, ROW_T, preferred_element_type=F32)


def build_kernel(src_hbm, dst_hbm, w_hbm, ma, mb, src_v, dst_v, w_v, row_v, lane_v, lane2_v, w2_v, left_v, ua, ub, *rest):
    rss, sem, rsem = rest[:NSM], rest[NSM], rest[NSM + 1]
    tiles = src_v.shape[0] // 8
    loads = [pltpu.make_async_copy(a, b, sem.at[k]) for k, (a, b) in enumerate(((src_hbm, src_v), (dst_hbm, dst_v), (w_hbm, w_v)))]
    for c in loads: c.start()
    def zero(i, c):
        z = jnp.zeros((256, 128), F32)
        rows = pl.ds(pl.multiple_of(i * 256, 256), 256)
        ma[rows, :] = z; mb[rows, :] = z
        return c
    lax.fori_loop(0, LAST // 256, zero, 0)
    for c in loads: c.wait()
    sub = lax.broadcasted_iota(jnp.int32, (8, 128), 0)
    def prep(t, left):
        tile = pl.ds(pl.multiple_of(t * 8, 8), 8)
        dst = dst_v[tile, :]
        row = ((dst >> 7) << 11) + src_v[tile, :]
        lane = (dst & 127).astype(F32)
        w = w_v[tile, :]
        seen = jnp.zeros((8, 128), F32); lane2 = seen; w2 = seen
        for d in range(1, 8):
            same = jnp.logical_and(row == pltpu.roll(row, d, axis=0), sub >= d)
            seen = seen + jnp.where(same, 1.0, 0.0)
            lane2 = lane2 + jnp.where(same, pltpu.roll(lane, d, axis=0), 0.0)
            w2 = w2 + jnp.where(same, pltpu.roll(w, d, axis=0), 0.0)
        late = seen > 1.5
        row_v[tile, :] = jnp.where(late, LAST, row)
        lane_v[tile, :] = lane
        lane2_v[tile, :] = lane2
        w2_v[tile, :] = w2
        mark = jnp.where(late, 1.0, 0.0)
        left_v[tile, :] = mark
        return left + mark
    left = lax.fori_loop(0, tiles, prep, jnp.zeros((8, 128), F32))
    n_left = jnp.sum(left)

    def rows_copy(t, rs, k):
        return pltpu.make_async_copy(row_v.at[pl.ds(pl.multiple_of(t * 8, 8), 8), :], rs, rsem.at[k])
    lanes = lax.broadcasted_iota(jnp.int32, (128, 128), 1).astype(F32)
    def cols(t):
        tile = pl.ds(pl.multiple_of(t * 8, 8), 8)
        return [r[tile, :].T for r in (lane_v, w_v, lane2_v, w2_v)]
    def make_u(cs, k, u):
        l1, w1, l2, w2 = [jnp.broadcast_to(c[:, k:k + 1], (128, 128)) for c in cs]
        u[k] = jnp.where(lanes == l1, w1, 0.0) + jnp.where(lanes == l2, w2, 0.0)
    def rmw_half(rs, u, hooks):
        pend = None
        for j in range(129):
            if j < 128:
                m = ma if j % 2 == 0 else mb
                rows = [rs[k, j] for k in range(8)]
                vals = [m[pl.ds(rows[k], 1), :] + u[k, pl.ds(j, 1), :] for k in range(8)]
            if pend is not None:
                pm, prow, pval = pend
                for k in range(8):
                    pm[pl.ds(prow[k], 1), :] = pval[k]
            if j < 128:
                pend = (m, rows, vals)
                if j % 16 == 0 and hooks: hooks[j // 16]()
    def half(t, nxt, cur_u, nxt_u, cur_rs):
        cs = cols(nxt)
        hooks = [functools.partial(make_u, cs, k, nxt_u) for k in range(8)]
        rmw_half(cur_rs, cur_u, hooks)
    cs = cols(0)
    for k in range(8): make_u(cs, k, ua)
    NS = len(rss)
    for q in range(NS - 1): rows_copy(q, rss[q], q).start()
    def body(i, c):
        for q in range(NS):
            t = NS * i + q
            rows_copy(t, rss[q], q).wait()
            rows_copy(jnp.minimum(t + NS - 1, tiles - 1), rss[(q + NS - 1) % NS], (q + NS - 1) % NS).start()
            half(t, jnp.minimum(t + 1, tiles - 1), (ua, ub)[q % 2], (ub, ua)[q % 2], rss[q])
        return c
    lax.fori_loop(0, tiles // NS, body, 0)
    for q in range(NS - 1): rows_copy(tiles - 1, rss[q], q).wait()

    pos = lax.broadcasted_iota(jnp.int32, (8 * tiles, 128), 0) * 128 + lax.broadcasted_iota(jnp.int32, (8 * tiles, 128), 1)
    lane_row = lax.broadcasted_iota(jnp.int32, (1, 128), 1)
    def one_left(i, c):
        p = jnp.min(jnp.where(left_v[...] > 0.5, pos, 8 * tiles * 128).astype(F32)).astype(jnp.int32)
        here = pos == p
        left_v[...] = jnp.where(here, 0.0, left_v[...])
        pick = lambda x: jnp.sum(jnp.where(here, x, 0.0))
        dst = pick(dst_v[...].astype(F32)).astype(jnp.int32)
        row = ((dst >> 7) << 11) + pick(src_v[...].astype(F32)).astype(jnp.int32)
        ma[pl.ds(row, 1), :] = ma[pl.ds(row, 1), :] + jnp.where(lane_row == (dst & 127), pick(w_v[...]), 0.0)
        return c
    lax.fori_loop(0, n_left.astype(jnp.int32), one_left, 0)


def build(src,dst,w):
    n=src.shape[0]; nb=n//128
    s2=lambda a:pltpu.with_memory_space_constraint(a.reshape(nb,128), pltpu.HBM)
    o=jax.ShapeDtypeStruct((LAST+8,128),F32)
    V=pl.BlockSpec(memory_space=pltpu.VMEM); H=pl.BlockSpec(memory_space=pltpu.HBM)
    S=pltpu.VMEM
    return pl.pallas_call(build_kernel, out_shape=[o]*2, in_specs=[H]*3, out_specs=[V]*2,
        scratch_shapes=[S((nb,128),jnp.int32)]*2+[S((nb,128),F32)]+[S((nb,128),jnp.int32)]+[S((nb,128),F32)]*4
          +[S((8,128,128),F32)]*2+[pltpu.SMEM((8,128),jnp.int32)]*NSM+[pltpu.SemaphoreType.DMA((3,)),pltpu.SemaphoreType.DMA((NSM,))],
        name="build", cost_estimate=pl.CostEstimate(flops=10**10, bytes_accessed=80 * 10**6, transcendentals=0), compiler_params=pltpu.CompilerParams(vmem_limit_bytes=36*1024*1024))(s2(src),s2(dst),s2(w))


def step_kernel(
    x_ref, w1_ref, w2_ref, send_ref, ma_ref, mb_ref, lab_ref, mask_ref,
    out_ref, small_ref,
    s0_ref, s1_ref, sb1, hp1, hn1, sb2, hp2, hn2, ga2, gb2, ra2, rb2, gb1, ra1, rb1,
    y_ref, hid_ref, part, rc, a1, rx, cnt, cntr, sml, smlr, own_ref, dy_ref, w2p, bh_ref, bm_ref, bl_ref, r0_ref, r1_ref, ssem, rsem, fsem, frsem, gsem, grsem,
):
    me = lax.axis_index(AXIS)
    num = 128
    core = lax.rem(me, 2)
    cx = lax.rem(me // 2, 4)
    cy = lax.rem(me // 8, 4)
    cz = me // 32
    away = lax.rem(me + num - 1 + 2 * core, num)
    twin = me + 1 - 2 * core
    dims = ((cx, 2), (cy, 8), (cz, 32))

    def peer(dim, d):
        c, stride = dims[dim]
        p = lax.rem(c + d, 4)
        return p, me + (p - c) * stride

    barrier = pltpu.get_barrier_semaphore()
    targets = [away, twin] + [peer(k, d)[1] for k in range(3) for d in (1, 2, 3)]
    for t in targets:
        pl.semaphore_signal(barrier, inc=1, device_id=(t,), device_id_type=pl.DeviceIdType.MESH)

    counter = [0]

    def copy(src, dst, dev):
        k = counter[0]
        counter[0] += 1
        c = pltpu.make_async_remote_copy(
            src_ref=src, dst_ref=dst, send_sem=ssem.at[k], recv_sem=rsem.at[k],
            device_id=(dev,), device_id_type=pl.DeviceIdType.MESH,
        )
        c.start()
        return c

    cnt[...] = jnp.broadcast_to(jnp.sum(mask_ref[...].astype(F32), axis=1, keepdims=True), (8, 128))

    def small_start(val, recv, stage):
        if stage == 0:
            return [copy(val, recv.at[0, 0], twin)]
        c, _ = dims[stage - 1]
        recv[stage, c] = val[...]
        return [copy(val, recv.at[stage, c], peer(stage - 1, d)[1]) for d in (1, 2, 3)]

    def small_end(copies, val, recv, stage):
        for c in copies:
            c.wait()
        if stage == 0:
            val[...] = val[...] + recv[0, 0]
        else:
            val[...] = (recv[stage, 0] + recv[stage, 1]) + (recv[stage, 2] + recv[stage, 3])


    w2p[...] = jnp.zeros((HID, HID), F32)
    w2p[0:19, :] = w2_ref[...]
    w2t = w2p[0:PADC, :].astype(BF16)
    w2n = w2p[...].T.astype(BF16)[:, 0:PADC]

    node = lax.broadcasted_iota(jnp.int32, (NODES, HALO), 0)
    s0_ref[...] = jnp.where(node == send_ref[pl.ds(1 - core, 1), :], 1.0, 0.0).astype(BF16)
    s1_ref[...] = jnp.where(node == send_ref[pl.ds(core, 1), :], 1.0, 0.0).astype(BF16)

    t1 = dot_n(x_ref[...], w1_ref[...].astype(BF16))
    t1 = t1.T.astype(BF16)
    sb1[1] = dot_n(t1, s1_ref[...]).astype(BF16)
    pl.semaphore_wait(barrier, len(targets))
    c_p = copy(sb1.at[1], hp1, away)
    sb1[0] = dot_n(t1, s0_ref[...]).astype(BF16)
    c_n = copy(sb1.at[0], hn1, twin)
    cc = small_start(cnt, cntr, 0)

    def agg(e, lo, hi):
        acc = dot_n(e, bl_ref[lo:hi, :])
        acc = acc + dot_n(e, bm_ref[lo:hi, :])
        return acc + dot_n(e, bh_ref[lo:hi, :])

    def split_block(first, source, blocks):
        def one(i, c):
            rows = pl.ds(pl.multiple_of((first + i) * 128, 128), 128)
            for j in range(NODES // 128):
                from_rows = pl.ds(pl.multiple_of(j * EXT + (source + i) * 128, 128), 128)
                h, m, l = split3(ma_ref[from_rows, :] + mb_ref[from_rows, :])
                cols = pl.ds(j * 128, 128)
                bh_ref[rows, cols] = h
                bm_ref[rows, cols] = m
                bl_ref[rows, cols] = l
            return c

        lax.fori_loop(0, blocks, one, 0)

    split_block(0, 0, 8)
    y_ref[...] = agg(t1, 0, NODES)
    split_block(12, 12 - 4 * core, 4)
    split_block(8, 8 + 4 * core, 4)
    column = lax.broadcasted_iota(jnp.int32, (HALO, NODES), 1).astype(F32)
    for k, r_ref in ((1 - core, r0_ref), (core, r1_ref)):
        ids = jnp.broadcast_to(send_ref[pl.ds(k, 1), :].astype(F32), (8, HALO)).T[:, 0:1]
        r_ref[...] = jnp.where(column == ids, 1.0, 0.0).astype(BF16)
    small_end(cc, cnt, cntr, 0)
    cc = small_start(cnt, cntr, 1)
    c_n.wait()
    y_ref[...] += agg(hn1[...], NODES + HALO, EXT)
    c_p.wait()
    y = y_ref[...] + agg(hp1[...], NODES, NODES + HALO)
    y_ref[...] = y
    small_end(cc, cnt, cntr, 1)
    cc = small_start(cnt, cntr, 2)
    hid = jnp.maximum(y, 0.0).astype(BF16)
    hid_ref[...] = hid
    t2 = dot_n(w2t, hid).astype(BF16)
    sb2[1] = dot_n(t2, s1_ref[...]).astype(BF16)
    c_p = copy(sb2.at[1], hp2, away)
    sb2[0] = dot_n(t2, s0_ref[...]).astype(BF16)
    c_n = copy(sb2.at[0], hn2, twin)
    z = agg(t2, 0, NODES)
    small_end(cc, cnt, cntr, 2)
    cc = small_start(cnt, cntr, 3)
    c_n.wait()
    z = z + agg(hn2[...], NODES + HALO, EXT)
    c_p.wait()
    z = z + agg(hp2[...], NODES, NODES + HALO)
    small_end(cc, cnt, cntr, 3)
    count = jnp.maximum(cnt[0:1, 0:1], 1.0)

    cls = lax.broadcasted_iota(jnp.int32, (PADC, NODES), 0)
    real = cls < 19
    mask = mask_ref[...].astype(F32)
    zm = jnp.where(real, z, -jnp.inf)
    top = jnp.max(zm, axis=0, keepdims=True)
    grown = jnp.where(real, jnp.exp(zm - top), 0.0)
    weight = jnp.sum(grown, axis=0, keepdims=True)
    norm = jnp.log(weight) + top
    hot = (cls == lab_ref[...]).astype(F32)
    picked = jnp.sum(z * hot, axis=0, keepdims=True)
    loss = jnp.sum(mask * (norm - picked), axis=1, keepdims=True)
    dz = (grown / weight - hot) * (mask / count)

    def agg_back(d, lo, hi):
        n = d.shape[0]
        dh, dm, dl = split3(d)
        rh = dot_t(jnp.concatenate([dh, dm, dl], axis=0), bh_ref[lo:hi, :])
        rm = dot_t(jnp.concatenate([dh, dm], axis=0), bm_ref[lo:hi, :])
        rl = dot_t(dh, bl_ref[lo:hi, :])
        return rh[0:n] + ((rh[n:2 * n] + rm[0:n]) + (rh[2 * n:3 * n] + (rm[n:2 * n] + rl)))

    def returned(r, s_rows):
        n = r.shape[0]
        t = dot_n(jnp.concatenate(split3(r), axis=0), s_rows)
        return t[0:n] + (t[n:2 * n] + t[2 * n:3 * n])

    c_p = []
    for h in range(2):
        ga2[h] = agg_back(dz, NODES + h * QTR, NODES + (h + 1) * QTR)
        c_p.append(copy(ga2.at[h], ra2.at[h], away))
    gb2[...] = agg_back(dz, NODES + HALO, EXT)
    c_n = copy(gb2, rb2, twin)
    own = agg_back(dz, 0, NODES)
    c_n.wait()
    own = own + returned(rb2[...], r0_ref[...])
    for h in range(2):
        c_p[h].wait()
        own = own + returned(ra2[h], r1_ref[pl.ds(h * QTR, QTR), :])
    dt2 = own.astype(BF16)
    g2 = dot_t(dt2, hid_ref[...])
    sml[...] = g2
    sml[24:32, :] = jnp.broadcast_to(loss, (8, 128))
    cs = small_start(sml, smlr, 0)
    dh = dot_n(w2n, dt2)
    dy_ref[...] = jnp.where(y_ref[...] > 0.0, dh, 0.0)
    back = []
    for side, land, dev in ((0, ra1, away), (1, rb1, twin)):
        for h in range(2):
            first = NODES + side * HALO + h * QTR
            gb1[side, h] = agg_back(dy_ref[...], first, first + QTR)
            back.append(copy(gb1.at[side, h], land.at[h], dev))
    small_end(cs, sml, smlr, 0)
    cs = small_start(sml, smlr, 1)
    own_ref[...] = agg_back(dy_ref[...], 0, NODES)
    small_end(cs, sml, smlr, 1)
    cs = small_start(sml, smlr, 2)
    for side, land, rows_ref in ((1, rb1, r0_ref), (0, ra1, r1_ref)):
        for h in range(2):
            back[2 * side + h].wait()
            own_ref[...] += returned(land[h], rows_ref[pl.ds(h * QTR, QTR), :])
    dt1 = own_ref[...].astype(BF16)

    mine = pl.ds(pl.multiple_of(core * 512, 512), 512)
    other = pl.ds(pl.multiple_of((1 - core) * 512, 512), 512)
    part[...] = dot_n(dt1, x_ref[:, other]).T
    swap = copy(part, rc, twin)
    small_end(cs, sml, smlr, 2)
    cs = small_start(sml, smlr, 3)
    own_half = dot_n(dt1, x_ref[:, mine]).T
    swap.wait()
    a1[...] = own_half + rc[...]

    chip = me // 2

    def rows_of(q):
        return pl.ds(pl.multiple_of(q * 8, 8), 8)

    spot = lax.rem(chip, 16)
    mine8 = pl.ds(pl.multiple_of(core * 512 + chip * 8, 8), 8)
    shifts = [(dz, dr) for dz in (2, 1, 3, 0) for dr in range(16) if dz + dr > 0]

    def far(dz, dr):
        q = lax.rem(cz + dz, 4) * 16 + lax.rem(spot + dr, 16)
        return dz * 16 + dr - 1, q, q * 2 + core

    def far_copy(dz, dr, gather):
        k, q, dev = far(dz, dr)
        src = out_ref.at[mine8] if gather else a1.at[rows_of(q)]
        return pltpu.make_async_remote_copy(
            src_ref=src, dst_ref=src if gather else rx.at[k],
            send_sem=(gsem if gather else fsem).at[k], recv_sem=(grsem if gather else frsem).at[k],
            device_id=(dev,), device_id_type=pl.DeviceIdType.MESH,
        )

    scatters = [far_copy(dz, dr, False) for dz, dr in shifts]
    for c in scatters:
        c.start()
    small_end(cs, sml, smlr, 3)
    for c in scatters:
        c.wait()
    total = [a1[rows_of(chip), :]] + [rx[k] for k in range(CHIPS - 1)]
    while len(total) > 1:
        total = [total[k] + total[k + 1] for k in range(0, len(total), 2)]
    out_ref[mine8, :] = total[0]
    gathers = {(dz, dr): far_copy(dz, dr, True) for dz, dr in shifts}
    for c in gathers.values():
        c.start()
    last = []
    for dz in (0, 1, 3, 2):
        for dr in range(16):
            if dz + dr > 0:
                gathers[dz, dr].wait()
        plane = pl.ds(pl.multiple_of(core * 512 + lax.rem(cz - dz + 4, 4) * 128, 128), 128)
        last.append(copy(out_ref.at[plane], out_ref.at[plane], twin))
    small_ref[...] = sml[...]
    small_ref[24:32, :] = sml[24:32, :] / count
    for c in last:
        c.wait()


def finish_kernel(one_in, small_in, loss_ref, one_ref, two_ref, two_v, sem):
    one = pltpu.make_async_copy(one_in, one_ref, sem.at[0])
    one.start()
    two_v[...] = small_in[0:19, :]
    two = pltpu.make_async_copy(two_v, two_ref, sem.at[1])
    two.start()
    loss_ref[0, 0] = jnp.max(small_in[24:25, :])
    one.wait()
    two.wait()


def finish(one, small):
    vmem = pl.BlockSpec(memory_space=pltpu.VMEM)
    hbm = pl.BlockSpec(memory_space=pltpu.HBM)
    return pl.pallas_call(
        finish_kernel,
        out_shape=[
            jax.ShapeDtypeStruct((1, 1), F32), jax.ShapeDtypeStruct(one.shape, F32), jax.ShapeDtypeStruct((19, HID), F32),
        ],
        in_specs=[vmem] * 2,
        out_specs=[pl.BlockSpec(memory_space=pltpu.SMEM), hbm, hbm],
        scratch_shapes=[pltpu.VMEM((19, HID), F32), pltpu.SemaphoreType.DMA((2,))],
        name="finish",
        compiler_params=pltpu.CompilerParams(vmem_limit_bytes=4 * 1024 * 1024),
    )(one, small)


def step(x, w_one, w_two, send_rows, src, dst, w, labels, mask):
    ma, mb = build(src, dst, w)
    vmem = pl.BlockSpec(memory_space=pltpu.VMEM)
    n_sem = 36
    V = pltpu.VMEM
    one, small = pl.pallas_call(
        step_kernel,
        out_shape=[
            jax.ShapeDtypeStruct((1024, HID), F32),
            jax.ShapeDtypeStruct((PADC, HID), F32),
        ],
        in_specs=[vmem] * 8,
        out_specs=[vmem] * 2,
        scratch_shapes=[
            V((NODES, HALO), BF16), V((NODES, HALO), BF16),
            V((2, HID, HALO), BF16), V((HID, HALO), BF16), V((HID, HALO), BF16),
            V((2, PADC, HALO), BF16), V((PADC, HALO), BF16), V((PADC, HALO), BF16),
            V((2, PADC, QTR), F32), V((PADC, HALO), F32), V((2, PADC, QTR), F32), V((PADC, HALO), F32),
            V((2, 2, HID, QTR), F32), V((2, HID, QTR), F32), V((2, HID, QTR), F32),
            V((HID, NODES), F32), V((HID, NODES), BF16),
            V((512, HID), F32), V((512, HID), F32), V((512, HID), F32),
            V((CHIPS - 1, 8, HID), F32),
            V((8, 128), F32), V((4, 4, 8, 128), F32), V((PADC, 128), F32), V((4, 4, PADC, 128), F32),
            V((HID, NODES), F32), V((HID, NODES), F32), V((HID, HID), F32),
            V((EXT, NODES), BF16), V((EXT, NODES), BF16), V((EXT, NODES), BF16),
            V((HALO, NODES), BF16), V((HALO, NODES), BF16),
            pltpu.SemaphoreType.DMA((n_sem,)), pltpu.SemaphoreType.DMA((n_sem,)),
            *[pltpu.SemaphoreType.DMA((CHIPS - 1,))] * 4,
        ],
        name="step",
        compiler_params=pltpu.CompilerParams(
            collective_id=0, has_side_effects=True, vmem_limit_bytes=31 * 1024 * 1024
        ),
    )(x, w_one, w_two.T, send_rows, ma, mb, labels.reshape(1, NODES), mask.reshape(1, NODES))
    loss, one, two = finish(one, small)
    return loss.reshape(()), one, two.T


def solution(mesh):
    row = P(AXIS)
    return jax.shard_map(
        step, mesh=mesh, in_specs=(row, P(), P(), row, row, row, row, row, row),
        out_specs=(P(), P(), P()), check_vma=False,
    )
```
